8 devices in a mesh: replica: 2 (over z, y), dp: 4 (over x, core).
Axes of the slice: x: 2, y: 2, z: 1, core: 2. Of those that a mesh axis runs over, the one named last changes fastest.
Arguments:
- x: bfloat16 [512, 2048], P(('replica', 'dp')), parts along dimension 0
- lengths: int32 [512], P(('replica', 'dp')), parts along dimension 0
- cache: bfloat16 [2, 512, 512, 576], P(None, ('replica', 'dp')), parts along dimension 1
- attn_gain: float32 [2, 2048], replicated
- ffn_gain: float32 [2, 2048], replicated
- w_query: bfloat16 [2, 2048, 9216], replicated
- w_attn_out: bfloat16 [2, 8192, 2048], replicated
- w_up: bfloat16 [2, 2048, 10944], P(None, None, 'dp')
- w_gate: bfloat16 [2, 2048, 10944], P(None, None, 'dp')
- w_down: bfloat16 [2, 10944, 2048], P(None, 'dp')
Outputs:
- output: bfloat16 [512, 2048], P(('replica', 'dp')), parts along dimension 0
There are 2 independent parts. The reference program is written for one: setup_inputs(seed, part) draws one part's arguments, and reference() takes and returns one part's arrays. A program takes and returns all parts, laid end to end along the dimension named above; an argument that names none is the same for every part.
All inputs are finite; a program needn't handle non-finite values.
Results may differ from the reference program's by a relative error of at most 0.02.
Values are sent between devices in bfloat16 or wider.
A program may use at most 1.25 GiB of HBM per device.

```python
import jax
import jax.numpy as jnp
from jax import lax

B_DEV = 64
GROUP_SIZE = 4
SEQ_LEN = 512
D_MODEL = 2048
FF_DIM = 10944
HEADS = 16
LATENT = 512
ROPE = 64
LAYERS = 2

NORM_EPS = 1e-6
BATCH = B_DEV * GROUP_SIZE
KV_DIM = LATENT + ROPE
SCORE_SCALE = (3 * ROPE) ** -0.5
LEN_FLOOR = max(1, SEQ_LEN // 16)
CAP_FLOOR = max(LEN_FLOOR, SEQ_LEN // 4)


def draw_lengths(key):
    cap_key, len_key, pick_key = jax.random.split(key, 3)
    caps = jax.random.randint(cap_key, (GROUP_SIZE,), CAP_FLOOR, SEQ_LEN + 1)
    full_dev = jax.random.randint(pick_key, (), 0, GROUP_SIZE)
    caps = jnp.where(jnp.arange(GROUP_SIZE) == full_dev, SEQ_LEN, caps)
    drawn = jax.random.randint(len_key, (GROUP_SIZE, B_DEV), LEN_FLOOR, caps[:, None] + 1)
    drawn = jnp.concatenate([drawn[:, 1:], caps[:, None]], axis=1)
    return jnp.sort(drawn, axis=1).reshape(BATCH).astype(jnp.int32)


def setup_inputs(seed: int = 0, part: int = 0) -> dict:
    part_key = jax.random.fold_in(jax.random.key(seed), part)
    x_key, len_key, cache_key = jax.random.split(part_key, 3)
    shared_keys = jax.random.split(jax.random.key(seed + 1), 7)
    wo_scale = (HEADS * LATENT) ** -0.5 * max(1.0, (SEQ_LEN / 64) ** 0.5)
    return {
        'x': jax.random.normal(x_key, (BATCH, D_MODEL), jnp.float32).astype(jnp.bfloat16),
        'lengths': draw_lengths(len_key),
        'cache': jax.random.normal(cache_key, (LAYERS, BATCH, SEQ_LEN, KV_DIM), jnp.float32).astype(jnp.bfloat16),
        'attn_gain': 0.5 + jax.random.uniform(shared_keys[0], (LAYERS, D_MODEL), jnp.float32),
        'ffn_gain': 0.5 + jax.random.uniform(shared_keys[1], (LAYERS, D_MODEL), jnp.float32),
        'w_query': (jax.random.normal(shared_keys[2], (LAYERS, D_MODEL, HEADS * KV_DIM), jnp.float32) * D_MODEL ** -0.5).astype(jnp.bfloat16),
        'w_attn_out': (jax.random.normal(shared_keys[3], (LAYERS, HEADS * LATENT, D_MODEL), jnp.float32) * wo_scale).astype(jnp.bfloat16),
        'w_up': (jax.random.normal(shared_keys[4], (LAYERS, D_MODEL, FF_DIM), jnp.float32) * D_MODEL ** -0.5).astype(jnp.bfloat16),
        'w_gate': (jax.random.normal(shared_keys[5], (LAYERS, D_MODEL, FF_DIM), jnp.float32) * D_MODEL ** -0.5).astype(jnp.bfloat16),
        'w_down': (jax.random.normal(shared_keys[6], (LAYERS, FF_DIM, D_MODEL), jnp.float32) * 2.0 * FF_DIM ** -0.5).astype(jnp.bfloat16),
    }


def rms_norm(rows, gain):
    rows_f = rows.astype(jnp.float32)
    mean_sq = jnp.mean(rows_f * rows_f, axis=-1, keepdims=True)
    return (rows_f * lax.rsqrt(mean_sq + NORM_EPS) * gain).astype(jnp.bfloat16)


def attention_layer(x_all, lengths, cache_l, gain, wq_l, wo_l):
    x_blocks = x_all.reshape(GROUP_SIZE, B_DEV, D_MODEL)
    len_blocks = lengths.reshape(GROUP_SIZE, B_DEV)
    cache_blocks = cache_l.reshape(GROUP_SIZE, B_DEV, SEQ_LEN, KV_DIM)
    positions = jnp.arange(SEQ_LEN)[None, None, :]

    def one_block(block):
        x_rows, len_rows, cache_rows = block
        normed = rms_norm(x_rows, gain)
        query = jnp.dot(normed, wq_l, preferred_element_type=jnp.float32).astype(jnp.bfloat16)
        query = query.reshape(B_DEV, HEADS, KV_DIM).astype(jnp.float32)
        cache_f = cache_rows.astype(jnp.float32)
        scores = jnp.einsum('bhc,btc->bht', query, cache_f) * SCORE_SCALE
        scores = jnp.where(positions < len_rows[:, None, None], scores, -jnp.inf)
        attn_probs = jax.nn.softmax(scores, axis=-1).astype(jnp.bfloat16).astype(jnp.float32)
        mixed = jnp.einsum('bht,btc->bhc', attn_probs, cache_f[:, :, :LATENT]).astype(jnp.bfloat16)
        attn_out = jnp.dot(mixed.reshape(B_DEV, HEADS * LATENT), wo_l, preferred_element_type=jnp.float32)
        return (x_rows.astype(jnp.float32) + attn_out).astype(jnp.bfloat16)

    return lax.map(one_block, (x_blocks, len_blocks, cache_blocks)).reshape(BATCH, D_MODEL)


def ffn_layer(x_all, gain, wu_l, wg_l, wd_l):
    normed = rms_norm(x_all, gain)
    gate_pre = jnp.dot(normed, wg_l, preferred_element_type=jnp.float32)
    up_pre = jnp.dot(normed, wu_l, preferred_element_type=jnp.float32)
    hidden = (jax.nn.silu(gate_pre) * up_pre).astype(jnp.bfloat16)
    ffn_out = jnp.dot(hidden, wd_l, preferred_element_type=jnp.float32)
    return (x_all.astype(jnp.float32) + ffn_out).astype(jnp.bfloat16)


def reference(x, lengths, cache, attn_gain, ffn_gain, w_query, w_attn_out, w_up, w_gate, w_down):
    def layer_step(x_cur, params):
        cache_l, gain_a, gain_f, wq_l, wo_l, wu_l, wg_l, wd_l = params
        x_cur = attention_layer(x_cur, lengths, cache_l, gain_a, wq_l, wo_l)
        x_cur = ffn_layer(x_cur, gain_f, wu_l, wg_l, wd_l)
        return x_cur, None

    x_final, _ = lax.scan(layer_step, x, (cache, attn_gain, ffn_gain, w_query, w_attn_out, w_up, w_gate, w_down))
    return x_final
```

```python
import functools

import jax
import jax.numpy as jnp
from jax import lax
from jax.experimental import pallas as pl
from jax.experimental.pallas import tpu as pltpu
from jax.sharding import PartitionSpec as P

NORM_EPS = 1e-6
SEQS = 8
SLOTS = 3
TBLK = 128
PARTS = 2


def rms_norm(rows, gain):
    rows_f = rows.astype(jnp.float32)
    mean_sq = jnp.mean(rows_f * rows_f, axis=-1, keepdims=True)
    return (rows_f * lax.rsqrt(mean_sq + NORM_EPS) * gain).astype(jnp.bfloat16)


def attention_kernel(layer, scale, len_ref, q_ref, cache_ref, o_ref, buf, score_buf, prob_buf, sem):
    rows, heads, kv_dim = q_ref.shape
    seq_len = cache_ref.shape[3]
    latent = o_ref.shape[2]
    groups = rows // SEQS
    max_blocks = seq_len // TBLK

    def blocks_of(group):
        longest = len_ref[group * SEQS]
        for i in range(1, SEQS):
            longest = jnp.maximum(longest, len_ref[group * SEQS + i])
        return lax.div(longest + (TBLK - 1), TBLK)

    def copy(group, slot, n):
        return pltpu.make_async_copy(
            cache_ref.at[layer, pl.ds(group * SEQS, SEQS), :, pl.ds(0, n * TBLK)],
            buf.at[slot, :, :, pl.ds(0, n * TBLK)],
            sem.at[slot],
        )

    def start(group, slot):
        blocks = blocks_of(group)
        for n in range(1, max_blocks + 1):

            @pl.when(blocks == n)
            def _():
                copy(group, slot, n).start()

    for group in range(min(SLOTS, groups)):
        start(group, group)

    def step(group, carry):
        slot = lax.rem(group, SLOTS)
        blocks = blocks_of(group)
        for n in range(1, max_blocks + 1):

            @pl.when(blocks == n)
            def _():
                copy(group, slot, n).wait()
                width = n * TBLK
                positions = lax.broadcasted_iota(jnp.int32, (heads, width), 1)
                for i in range(SEQS):
                    row = group * SEQS + i
                    score_buf[pl.ds(i * heads, heads), pl.ds(0, width)] = jnp.dot(
                        q_ref[row], buf[slot, i, :, pl.ds(0, width)], preferred_element_type=jnp.float32
                    )
                for part in range(PARTS):
                    size = SEQS // PARTS
                    for i in range(part * size, (part + 1) * size):
                        row = group * SEQS + i
                        scores = score_buf[pl.ds(i * heads, heads), pl.ds(0, width)]
                        scores = jnp.where(positions < len_ref[row], scores * scale, -jnp.inf)
                        top = jnp.max(scores, axis=-1, keepdims=True)
                        probs = jnp.exp(scores - top)
                        probs = probs / jnp.sum(probs, axis=-1, keepdims=True)
                        prob_buf[pl.ds(i * heads, heads), pl.ds(0, width)] = probs.astype(jnp.bfloat16)
                    for i in range(part * size, (part + 1) * size):
                        row = group * SEQS + i
                        mixed = lax.dot_general(
                            prob_buf[pl.ds(i * heads, heads), pl.ds(0, width)],
                            buf[slot, i, pl.ds(0, latent), pl.ds(0, width)],
                            (((1,), (1,)), ((), ())),
                            preferred_element_type=jnp.float32,
                        )
                        o_ref[row] = mixed.astype(jnp.bfloat16)

        @pl.when(group + SLOTS < groups)
        def _():
            start(group + SLOTS, slot)

        return carry

    lax.fori_loop(0, groups, step, 0)


def attention(layer, q, lengths, cache_t, latent):
    rows, heads, kv_dim = q.shape
    seq_len = cache_t.shape[3]
    scale = (3 * (kv_dim - latent)) ** -0.5
    return pl.pallas_call(
        functools.partial(attention_kernel, layer, scale),
        out_shape=jax.ShapeDtypeStruct((rows, heads, latent), jnp.bfloat16),
        in_specs=[
            pl.BlockSpec(memory_space=pltpu.SMEM),
            pl.BlockSpec(memory_space=pltpu.VMEM),
            pl.BlockSpec(memory_space=pl.ANY),
        ],
        out_specs=pl.BlockSpec(memory_space=pltpu.VMEM),
        scratch_shapes=[
            pltpu.VMEM((SLOTS, SEQS, kv_dim, seq_len), jnp.bfloat16),
            pltpu.VMEM((SEQS * heads, seq_len), jnp.float32),
            pltpu.VMEM((SEQS * heads, seq_len), jnp.bfloat16),
            pltpu.SemaphoreType.DMA((SLOTS,)),
        ],
        compiler_params=pltpu.CompilerParams(vmem_limit_bytes=40 * 1024 * 1024),
        name=f"attention_{layer}",
    )(lengths, q, cache_t)


def solution(mesh):
    row_axes = ('replica', 'dp')

    def local_step(x_rows, len_rows, cache, attn_gain, ffn_gain, w_query, w_attn_out, w_up, w_gate, w_down):
        kv_dim = cache.shape[3]
        heads = w_query.shape[2] // kv_dim
        latent = w_attn_out.shape[1] // heads
        rows = x_rows.shape[0]
        cache_t = jnp.swapaxes(cache, 2, 3)
        for layer_idx in range(cache.shape[0]):
            normed = rms_norm(x_rows, attn_gain[layer_idx])
            query = jnp.dot(normed, w_query[layer_idx], preferred_element_type=jnp.float32).astype(jnp.bfloat16)
            mixed = attention(layer_idx, query.reshape(rows, heads, kv_dim), len_rows, cache_t, latent)
            attn_out = jnp.dot(mixed.reshape(rows, heads * latent), w_attn_out[layer_idx], preferred_element_type=jnp.float32)
            x_rows = (x_rows.astype(jnp.float32) + attn_out).astype(jnp.bfloat16)
            normed = rms_norm(x_rows, ffn_gain[layer_idx])
            gathered = lax.all_gather(normed, 'dp', axis=0, tiled=True)
            gate_pre = jnp.dot(gathered, w_gate[layer_idx], preferred_element_type=jnp.float32)
            up_pre = jnp.dot(gathered, w_up[layer_idx], preferred_element_type=jnp.float32)
            hidden = (jax.nn.silu(gate_pre) * up_pre).astype(jnp.bfloat16)
            partial_out = jnp.dot(hidden, w_down[layer_idx], preferred_element_type=jnp.float32)
            ffn_rows = lax.psum_scatter(partial_out, 'dp', scatter_dimension=0, tiled=True)
            x_rows = (x_rows.astype(jnp.float32) + ffn_rows).astype(jnp.bfloat16)
        return x_rows

    return jax.shard_map(
        local_step,
        mesh=mesh,
        in_specs=(P(row_axes, None), P(row_axes), P(None, row_axes, None, None), P(), P(), P(), P(),
                  P(None, None, 'dp'), P(None, None, 'dp'), P(None, 'dp', None)),
        out_specs=P(row_axes, None),
        check_vma=False,
    )
```

```python
import functools

import jax
import jax.numpy as jnp
from jax import lax
from jax.experimental import pallas as pl
from jax.experimental.pallas import tpu as pltpu
from jax.sharding import PartitionSpec as P

NORM_EPS = 1e-6
SEQS = 8
SLOTS = 3
TBLK = 128
PARTS = 2


def rms_norm(rows, gain):
    rows_f = rows.astype(jnp.float32)
    mean_sq = jnp.mean(rows_f * rows_f, axis=-1, keepdims=True)
    return (rows_f * lax.rsqrt(mean_sq + NORM_EPS) * gain).astype(jnp.bfloat16)


def attention_kernel(layer, scale, len_ref, q_ref, cache_ref, o_ref, buf, score_buf, prob_buf, sem):
    rows, heads, kv_dim = q_ref.shape
    seq_len = cache_ref.shape[3]
    latent = o_ref.shape[2]
    groups = rows // SEQS
    max_blocks = seq_len // TBLK

    def blocks_of(group):
        longest = len_ref[group * SEQS]
        for i in range(1, SEQS):
            longest = jnp.maximum(longest, len_ref[group * SEQS + i])
        return lax.div(longest + (TBLK - 1), TBLK)

    def copy(group, slot, n):
        return pltpu.make_async_copy(
            cache_ref.at[layer, pl.ds(group * SEQS, SEQS), :, pl.ds(0, n * TBLK)],
            buf.at[slot, :, :, pl.ds(0, n * TBLK)],
            sem.at[slot],
        )

    def start(group, slot):
        blocks = blocks_of(group)
        for n in range(1, max_blocks + 1):

            @pl.when(blocks == n)
            def _():
                copy(group, slot, n).start()

    for group in range(min(SLOTS, groups)):
        start(group, group)

    def step(group, carry):
        slot = lax.rem(group, SLOTS)
        blocks = blocks_of(group)
        for n in range(1, max_blocks + 1):

            @pl.when(blocks == n)
            def _():
                copy(group, slot, n).wait()
                width = n * TBLK
                positions = lax.broadcasted_iota(jnp.int32, (heads, width), 1)
                for i in range(SEQS):
                    row = group * SEQS + i
                    score_buf[pl.ds(i * heads, heads), pl.ds(0, width)] = jnp.dot(
                        q_ref[row], buf[slot, i, :, pl.ds(0, width)], preferred_element_type=jnp.float32
                    )
                for part in range(PARTS):
                    size = SEQS // PARTS
                    for i in range(part * size, (part + 1) * size):
                        row = group * SEQS + i
                        scores = score_buf[pl.ds(i * heads, heads), pl.ds(0, width)]
                        scores = jnp.where(positions < len_ref[row], scores * scale, -jnp.inf)
                        top = jnp.max(scores, axis=-1, keepdims=True)
                        probs = jnp.exp(scores - top)
                        probs = probs / jnp.sum(probs, axis=-1, keepdims=True)
                        prob_buf[pl.ds(i * heads, heads), pl.ds(0, width)] = probs.astype(jnp.bfloat16)
                    for i in range(part * size, (part + 1) * size):
                        row = group * SEQS + i
                        mixed = lax.dot_general(
                            prob_buf[pl.ds(i * heads, heads), pl.ds(0, width)],
                            buf[slot, i, pl.ds(0, latent), pl.ds(0, width)],
                            (((1,), (1,)), ((), ())),
                            preferred_element_type=jnp.float32,
                        )
                        o_ref[row] = mixed.astype(jnp.bfloat16)

        @pl.when(group + SLOTS < groups)
        def _():
            start(group + SLOTS, slot)

        return carry

    lax.fori_loop(0, groups, step, 0)


def attention(layer, q, lengths, cache_t, latent):
    rows, heads, kv_dim = q.shape
    seq_len = cache_t.shape[3]
    scale = (3 * (kv_dim - latent)) ** -0.5
    return pl.pallas_call(
        functools.partial(attention_kernel, layer, scale),
        out_shape=jax.ShapeDtypeStruct((rows, heads, latent), jnp.bfloat16),
        in_specs=[
            pl.BlockSpec(memory_space=pltpu.SMEM),
            pl.BlockSpec(memory_space=pltpu.VMEM),
            pl.BlockSpec(memory_space=pl.ANY),
        ],
        out_specs=pl.BlockSpec(memory_space=pltpu.VMEM),
        scratch_shapes=[
            pltpu.VMEM((SLOTS, SEQS, kv_dim, seq_len), jnp.bfloat16),
            pltpu.VMEM((SEQS * heads, seq_len), jnp.float32),
            pltpu.VMEM((SEQS * heads, seq_len), jnp.bfloat16),
            pltpu.SemaphoreType.DMA((SLOTS,)),
        ],
        compiler_params=pltpu.CompilerParams(vmem_limit_bytes=40 * 1024 * 1024),
        name=f"attention_{layer}",
    )(lengths, q, cache_t)


MESH = pl.DeviceIdType.MESH
COLS = 256
HID = 512


def tail_kernel(
    layer, o_hbm, x_hbm, gain_ref, wo_hbm, wg_hbm, wu_hbm, wd_hbm, out_ref,
    o_all, x_old, wo_buf, wg, wu, wd, x_mid, g_all, a_all, p_other, p_own, part_in, pair_sum, cross_in, own_in,
    in_sem, wo_sem, w_sem, wd_sem, o_send, o_recv, xo_send, xo_recv, xp_send, xp_recv, xc_send, xc_recv, xf_send, xf_recv,
    p1_send, p1_recv, p2_send, p2_recv, p3_send, p3_recv,
):
    rows, d_model = x_hbm.shape
    chip_rows = 2 * rows
    half = d_model // 2
    hidden = wd_hbm.shape[1]
    slots = wo_buf.shape[0]
    x_pieces = half // COLS
    out_pieces = d_model // COLS
    full_steps = hidden // HID
    rest = hidden - full_steps * HID

    me = lax.axis_index('dp')
    core = lax.rem(me, 2)
    partner = me + 1 - 2 * core
    across = lax.rem(me + 2, 4)
    other_core = 1 - core
    my_rows = pl.ds(pl.multiple_of(core * rows, rows), rows)
    partner_rows = pl.ds(pl.multiple_of(other_core * rows, rows), rows)

    def remote(src, dst, send, recv, device):
        return pltpu.make_async_remote_copy(
            src_ref=src, dst_ref=dst, send_sem=send, recv_sem=recv, device_id={'dp': device}, device_id_type=MESH
        )

    def wo_copy(j):
        columns = pl.ds(pl.multiple_of(core * half + j * COLS, COLS), COLS)
        return pltpu.make_async_copy(wo_hbm.at[layer, :, columns], wo_buf.at[j % slots], wo_sem.at[j % slots])

    def up_copies(i):
        size = HID if i < full_steps else rest
        window = pl.ds(i * HID, size)
        return (
            pltpu.make_async_copy(wg_hbm.at[layer, window], wg.at[window], w_sem.at[0, i]),
            pltpu.make_async_copy(wu_hbm.at[layer, window], wu.at[window], w_sem.at[1, i]),
        )

    def down_copy(n):
        columns = pl.ds(n * COLS, COLS)
        return pltpu.make_async_copy(wd_hbm.at[layer, :, columns], wd.at[n], wd_sem.at[n])

    o_own = pltpu.make_async_copy(o_hbm, o_all.at[my_rows], in_sem.at[0])
    x_own = pltpu.make_async_copy(
        x_hbm.at[:, pl.ds(pl.multiple_of(core * half, half), half)], x_old.at[my_rows], in_sem.at[1]
    )
    o_own.start()
    x_own.start()
    for j in range(min(slots, x_pieces)):
        wo_copy(j).start()

    barrier = pltpu.get_barrier_semaphore()
    for peer in (partner, across):
        pl.semaphore_signal(barrier, inc=1, device_id={'dp': peer}, device_id_type=MESH)
    pl.semaphore_wait(barrier, 2)

    o_out = remote(o_hbm, o_all.at[my_rows], o_send, o_recv, partner)
    x_out = remote(
        x_hbm.at[:, pl.ds(pl.multiple_of(other_core * half, half), half)], x_old.at[my_rows], xo_send, xo_recv, partner
    )
    o_out.start()
    x_out.start()
    o_own.wait()
    x_own.wait()
    o_out.wait_recv()
    x_out.wait_recv()

    def to_partner(j):
        piece = x_mid.at[core, pl.ds(0, chip_rows), pl.ds(j * COLS, COLS)]
        return remote(piece, piece, xp_send.at[j], xp_recv.at[j], partner)

    def to_across(j):
        src = x_mid.at[core, pl.ds(0, chip_rows), pl.ds(j * COLS, COLS)]
        dst = x_mid.at[core, pl.ds(chip_rows, chip_rows), pl.ds(j * COLS, COLS)]
        return remote(src, dst, xc_send.at[j], xc_recv.at[j], across)

    def forward(j):
        piece = x_mid.at[core, pl.ds(chip_rows, chip_rows), pl.ds(j * COLS, COLS)]
        return remote(piece, piece, xf_send.at[j], xf_recv.at[j], partner)

    pending = [c for i in range(full_steps + (rest > 0)) for c in up_copies(i)] + [down_copy(n) for n in range(out_pieces)]
    quota = -(-len(pending) // x_pieces)
    for j in range(x_pieces):
        wo_copy(j).wait()
        product = jnp.dot(o_all[...], wo_buf[j % slots], preferred_element_type=jnp.float32)
        columns = pl.ds(j * COLS, COLS)
        x_mid[core, pl.ds(0, chip_rows), columns] = (x_old[:, columns].astype(jnp.float32) + product).astype(jnp.bfloat16)
        to_across(j).start()
        to_partner(j).start()
        if j + slots < x_pieces:
            wo_copy(j + slots).start()
        for c in pending[j * quota : (j + 1) * quota]:
            c.start()

    def normalize(start):
        window = pl.ds(start, chip_rows)
        halves = [x_mid[h, window, :].astype(jnp.float32) for h in range(2)]
        total = sum(jnp.sum(v * v, axis=-1, keepdims=True) for v in halves)
        factor = lax.rsqrt(total * (1.0 / d_model) + NORM_EPS)
        for h in range(2):
            gain = gain_ref[pl.ds(layer, 1), pl.ds(h * half, half)]
            g_all[window, pl.ds(h * half, half)] = (halves[h] * factor * gain).astype(jnp.bfloat16)

    for j in range(x_pieces):
        to_partner(j).wait_recv()
    normalize(0)
    for j in range(x_pieces):
        to_across(j).wait_recv()
        forward(j).start()
    for j in range(x_pieces):
        forward(j).wait_recv()
    normalize(chip_rows)

    def gate_up(i, start, size):
        window = pl.ds(start, size)
        dims = (((1,), (1,)), ((), ()))
        gate = lax.dot_general(g_all[...], wg[window, :], dims, preferred_element_type=jnp.float32)
        up = lax.dot_general(g_all[...], wu[window, :], dims, preferred_element_type=jnp.float32)
        a_all[:, window] = (jax.nn.silu(gate) * up).astype(jnp.bfloat16)

    def up_wait(i, start, size):
        window = pl.ds(start, size)
        pltpu.make_async_copy(wg_hbm.at[layer, window], wg.at[window], w_sem.at[0, i]).wait()
        pltpu.make_async_copy(wu_hbm.at[layer, window], wu.at[window], w_sem.at[1, i]).wait()

    def up_step(i, carry):
        start = pl.multiple_of(i * HID, HID)
        up_wait(i, start, HID)
        gate_up(i, start, HID)
        return carry

    lax.fori_loop(0, full_steps, up_step, 0)
    if rest:
        up_wait(full_steps, full_steps * HID, rest)
        gate_up(full_steps, full_steps * HID, rest)

    def pair_other(n):
        return remote(p_other.at[n, partner_rows], part_in.at[n], p1_send.at[n], p1_recv.at[n], partner)

    def cross(n):
        return remote(pair_sum.at[n], cross_in.at[n], p2_send.at[n], p2_recv.at[n], across)

    def pair_own(n):
        return remote(p_own.at[n, partner_rows], own_in.at[n], p3_send.at[n], p3_recv.at[n], partner)

    def send_sum(n):
        pair_other(n).wait_recv()
        pair_sum[n] = p_other[n, my_rows] + part_in[n]
        cross(n).start()

    def other_step(n, carry):
        columns = pl.ds(pl.multiple_of(n * COLS, COLS), COLS)
        pltpu.make_async_copy(wd_hbm.at[layer, :, columns], wd.at[n], wd_sem.at[n]).wait()
        p_other[n] = jnp.dot(a_all[pl.ds(chip_rows, chip_rows), :], wd[n], preferred_element_type=jnp.float32)
        pair_other(n).start()

        @pl.when(n >= 2)
        def _():
            send_sum(n - 2)

        return carry

    lax.fori_loop(0, out_pieces, other_step, 0)

    def own_step(n, carry):
        @pl.when(n < 2)
        def _():
            send_sum(n + out_pieces - 2)

        p_own[n] = jnp.dot(a_all[pl.ds(0, chip_rows), :], wd[n], preferred_element_type=jnp.float32)
        pair_own(n).start()
        return carry

    lax.fori_loop(0, out_pieces, own_step, 0)

    per_half = half // COLS
    for n in range(out_pieces):
        pair_own(n).wait_recv()
        cross(n).wait_recv()
        h, columns = n // per_half, pl.ds((n % per_half) * COLS, COLS)
        total = (p_own[n, my_rows] + own_in[n]) + cross_in[n]
        out_ref[:, pl.ds(n * COLS, COLS)] = (x_mid[h, my_rows, columns].astype(jnp.float32) + total).astype(jnp.bfloat16)

    o_out.wait_send()
    x_out.wait_send()
    for j in range(x_pieces):
        to_partner(j).wait_send()
        to_across(j).wait_send()
        forward(j).wait_send()
    for n in range(out_pieces):
        pair_other(n).wait_send()
        cross(n).wait_send()
        pair_own(n).wait_send()


def tail(layer, o, x, gain, wo, wg_t, wu_t, wd):
    rows, d_model = x.shape
    hidden = wd.shape[1]
    width = o.shape[1]
    half = d_model // 2
    x_pieces, out_pieces = half // COLS, d_model // COLS
    dma = pltpu.SemaphoreType.DMA
    steps = -(-hidden // HID)
    any_space = pl.BlockSpec(memory_space=pl.ANY)
    vmem = pl.BlockSpec(memory_space=pltpu.VMEM)
    return pl.pallas_call(
        functools.partial(tail_kernel, layer),
        out_shape=jax.ShapeDtypeStruct((rows, d_model), jnp.bfloat16),
        in_specs=[any_space, any_space, vmem, any_space, any_space, any_space, any_space],
        out_specs=vmem,
        scratch_shapes=[
            pltpu.VMEM((2 * rows, width), jnp.bfloat16),
            pltpu.VMEM((2 * rows, half), jnp.bfloat16),
            pltpu.VMEM((3, width, COLS), jnp.bfloat16),
            pltpu.VMEM((hidden, d_model), jnp.bfloat16),
            pltpu.VMEM((hidden, d_model), jnp.bfloat16),
            pltpu.VMEM((out_pieces, hidden, COLS), jnp.bfloat16),
            pltpu.VMEM((2, 4 * rows, half), jnp.bfloat16),
            pltpu.VMEM((4 * rows, d_model), jnp.bfloat16),
            pltpu.VMEM((4 * rows, hidden), jnp.bfloat16),
            pltpu.VMEM((out_pieces, 2 * rows, COLS), jnp.float32),
            pltpu.VMEM((out_pieces, 2 * rows, COLS), jnp.float32),
            pltpu.VMEM((out_pieces, rows, COLS), jnp.float32),
            pltpu.VMEM((out_pieces, rows, COLS), jnp.float32),
            pltpu.VMEM((out_pieces, rows, COLS), jnp.float32),
            pltpu.VMEM((out_pieces, rows, COLS), jnp.float32),
            dma((2,)), dma((3,)), dma((2, steps)), dma((out_pieces,)),
            dma, dma, dma, dma,
            dma((x_pieces,)), dma((x_pieces,)), dma((x_pieces,)), dma((x_pieces,)), dma((x_pieces,)), dma((x_pieces,)),
            dma((out_pieces,)), dma((out_pieces,)), dma((out_pieces,)), dma((out_pieces,)), dma((out_pieces,)), dma((out_pieces,)),
        ],
        compiler_params=pltpu.CompilerParams(
            collective_id=layer, has_side_effects=True, vmem_limit_bytes=63 * 1024 * 1024
        ),
        name=f"tail_{layer}",
    )(o, x, gain, wo, wg_t, wu_t, wd)


def solution(mesh):
    row_axes = ('replica', 'dp')

    def local_step(x_rows, len_rows, cache, attn_gain, ffn_gain, w_query, w_attn_out, w_up, w_gate, w_down):
        kv_dim = cache.shape[3]
        heads = w_query.shape[2] // kv_dim
        latent = w_attn_out.shape[1] // heads
        rows = x_rows.shape[0]
        cache_t = jnp.swapaxes(cache, 2, 3)
        up_t, gate_t = jnp.swapaxes(w_up, 1, 2), jnp.swapaxes(w_gate, 1, 2)
        for layer_idx in range(cache.shape[0]):
            normed = rms_norm(x_rows, attn_gain[layer_idx])
            query = jnp.dot(normed, w_query[layer_idx], preferred_element_type=jnp.float32).astype(jnp.bfloat16)
            mixed = attention(layer_idx, query.reshape(rows, heads, kv_dim), len_rows, cache_t, latent)
            x_rows = tail(layer_idx, mixed.reshape(rows, heads * latent), x_rows, ffn_gain, w_attn_out, gate_t, up_t, w_down)
        return x_rows

    return jax.shard_map(
        local_step,
        mesh=mesh,
        in_specs=(P(row_axes, None), P(row_axes), P(None, row_axes, None, None), P(), P(), P(), P(),
                  P(None, None, 'dp'), P(None, None, 'dp'), P(None, 'dp', None)),
        out_specs=P(row_axes, None),
        check_vma=False,
    )
```

```python
import functools

import jax
import jax.numpy as jnp
from jax import lax
from jax.experimental import pallas as pl
from jax.experimental.pallas import tpu as pltpu
from jax.sharding import PartitionSpec as P

NORM_EPS = 1e-6
MESH = pl.DeviceIdType.MESH
SEQS = 8
SLOTS = 3
TBLK = 128
PARTS = 2
COLS = 256
HID = 512
DOWN = 512
O_PARTS = 4
MIB = 1024 * 1024
LANES = 128
BULK = 1


def remote_copy(src, dst, send, recv, device):
    return pltpu.make_async_remote_copy(
        src_ref=src, dst_ref=dst, send_sem=send, recv_sem=recv, device_id={'dp': device}, device_id_type=MESH
    )


def enter(*peers):
    barrier = pltpu.get_barrier_semaphore()
    for peer in peers:
        pl.semaphore_signal(barrier, inc=1, device_id={'dp': peer}, device_id_type=MESH)
    pl.semaphore_wait(barrier, len(peers))


def rms_scaled(rows, gain):
    rows_f = rows.astype(jnp.float32)
    mean_sq = jnp.mean(rows_f * rows_f, axis=-1, keepdims=True)
    return (rows_f * lax.rsqrt(mean_sq + NORM_EPS) * gain).astype(jnp.bfloat16)


def project_q(h_ref, weights, core, partner, q_ref, q_send, send_sem, recv_sem):
    rows = q_send.shape[2] // 2
    kv_dim = weights[0][1].shape[1] // 2
    pairs = len(weights)

    def give(p):
        heads = pl.ds(pl.multiple_of((core * pairs + p) * 2 * rows, 2 * rows), 2 * rows)
        return remote_copy(q_send.at[p], q_ref.at[:, heads], send_sem.at[p], recv_sem.at[p], partner)

    for p, (wait, weight) in enumerate(weights):
        wait()
        q = jnp.dot(h_ref[...], weight[...], preferred_element_type=jnp.float32)
        q = q.astype(jnp.bfloat16).astype(jnp.float32)
        for e in range(2):
            own = pl.ds(pl.multiple_of((core * pairs + p) * 2 * rows + e * rows, rows), rows)
            for c in range(q_ref.shape[0]):
                size = min(LANES, kv_dim - c * LANES)
                part = q[:, e * kv_dim + c * LANES :][:, :size]
                q_ref[c, own, pl.ds(0, size)] = part[:rows]
                q_send[p, c, pl.ds(e * rows, rows), pl.ds(0, size)] = part[rows:]
        give(p).start()
    return [give(p) for p in range(pairs)]


def head_kernel(x_hbm, gain_hbm, wq_hbm, q_ref, x_ref, gain_ref, x_in, h_ref, wq, q_send, in_sem, wq_sem, x_send, x_recv, q_ssem, q_rsem):
    rows = x_hbm.shape[0]
    width = wq.shape[2]
    pairs = wq.shape[0]
    me = lax.axis_index('dp')
    core = lax.rem(me, 2)
    partner = me + 1 - 2 * core

    def wq_copy(p):
        columns = pl.ds(pl.multiple_of((core * pairs + p) * width, 128), width)
        return pltpu.make_async_copy(wq_hbm.at[0, :, columns], wq.at[p], wq_sem.at[p])

    x_own = pltpu.make_async_copy(x_hbm, x_ref, in_sem.at[0])
    gain_own = pltpu.make_async_copy(gain_hbm, gain_ref, in_sem.at[1])
    x_own.start()
    gain_own.start()
    for p in range(pairs):
        wq_copy(p).start(priority=BULK)
    x_own.wait()
    gain_own.wait()
    enter(partner)
    swap = remote_copy(x_ref, x_in, x_send, x_recv, partner)
    swap.start()
    h_ref[pl.ds(0, rows), :] = rms_scaled(x_ref[...], gain_ref[pl.ds(0, 1), :])
    swap.wait_recv()
    h_ref[pl.ds(rows, rows), :] = rms_scaled(x_in[...], gain_ref[pl.ds(0, 1), :])
    weights = [(wq_copy(p).wait, wq.at[p]) for p in range(pairs)]
    gives = project_q(h_ref, weights, core, partner, q_ref, q_send, q_ssem, q_rsem)
    swap.wait_send()
    for give in gives:
        give.wait()


def head(x, gain, wq, heads):
    rows, d_model = x.shape
    kv_dim = wq.shape[2] // heads
    pairs = heads // 4
    dma = pltpu.SemaphoreType.DMA
    vmem = pl.BlockSpec(memory_space=pltpu.VMEM)
    return pl.pallas_call(
        head_kernel,
        out_shape=jax.ShapeDtypeStruct((-(-kv_dim // LANES), heads * rows, LANES), jnp.float32),
        in_specs=[pl.BlockSpec(memory_space=pl.ANY)] * 3,
        out_specs=vmem,
        scratch_shapes=[
            pltpu.VMEM((rows, d_model), jnp.bfloat16),
            pltpu.VMEM(gain.shape, jnp.float32),
            pltpu.VMEM((rows, d_model), jnp.bfloat16),
            pltpu.VMEM((2 * rows, d_model), jnp.bfloat16),
            pltpu.VMEM((pairs, d_model, 2 * kv_dim), jnp.bfloat16),
            pltpu.VMEM((pairs, -(-kv_dim // LANES), 2 * rows, LANES), jnp.float32),
            dma((2,)), dma((pairs,)), dma, dma, dma((pairs,)), dma((pairs,)),
        ],
        compiler_params=pltpu.CompilerParams(collective_id=7, has_side_effects=True, vmem_limit_bytes=48 * MIB),
        name='head',
    )(x, gain, wq)


def attention_kernel(layer, scale, len_ref, q_ref, cache_ref, o_ref, buf, score_buf, prob_buf, o_buf, sem):
    rows = o_ref.shape[0]
    heads = q_ref.shape[1] // rows
    kv_dim, seq_len = cache_ref.shape[2:]
    latent = o_ref.shape[1] // heads
    groups = rows // SEQS
    max_blocks = seq_len // TBLK

    def blocks_of(group):
        longest = len_ref[group * SEQS]
        for i in range(1, SEQS):
            longest = jnp.maximum(longest, len_ref[group * SEQS + i])
        return lax.div(longest + (TBLK - 1), TBLK)

    def copy(group, slot, n):
        return pltpu.make_async_copy(
            cache_ref.at[layer, pl.ds(group * SEQS, SEQS), :, pl.ds(0, n * TBLK)],
            buf.at[slot, :, :, pl.ds(0, n * TBLK)],
            sem.at[slot],
        )

    def start(group, slot):
        blocks = blocks_of(group)
        for n in range(1, max_blocks + 1):

            @pl.when(blocks == n)
            def _():
                copy(group, slot, n).start()

    for group in range(min(SLOTS, groups)):
        start(group, group)

    def step(group, carry):
        slot = lax.rem(group, SLOTS)
        blocks = blocks_of(group)
        for n in range(1, max_blocks + 1):

            @pl.when(blocks == n)
            def _():
                copy(group, slot, n).wait()
                width = n * TBLK
                positions = lax.broadcasted_iota(jnp.int32, (heads, width), 1)
                for i in range(SEQS):
                    row = group * SEQS + i
                    query = [q_ref[c, pl.ds(row, heads, stride=rows), :] for c in range(q_ref.shape[0])]
                    query = jnp.concatenate(query, axis=1)[:, :kv_dim].astype(jnp.bfloat16)
                    score_buf[pl.ds(i * heads, heads), pl.ds(0, width)] = jnp.dot(
                        query, buf[slot, i, :, pl.ds(0, width)], preferred_element_type=jnp.float32
                    )
                for part in range(PARTS):
                    size = SEQS // PARTS
                    for i in range(part * size, (part + 1) * size):
                        row = group * SEQS + i
                        scores = score_buf[pl.ds(i * heads, heads), pl.ds(0, width)]
                        scores = jnp.where(positions < len_ref[row], scores * scale, -jnp.inf)
                        top = jnp.max(scores, axis=-1, keepdims=True)
                        probs = jnp.exp(scores - top)
                        probs = probs / jnp.sum(probs, axis=-1, keepdims=True)
                        prob_buf[pl.ds(i * heads, heads), pl.ds(0, width)] = probs.astype(jnp.bfloat16)
                    for i in range(part * size, (part + 1) * size):
                        row = group * SEQS + i
                        mixed = lax.dot_general(
                            prob_buf[pl.ds(i * heads, heads), pl.ds(0, width)],
                            buf[slot, i, pl.ds(0, latent), pl.ds(0, width)],
                            (((1,), (1,)), ((), ())),
                            preferred_element_type=jnp.float32,
                        )
                        for c in range(latent // LANES):
                            place = pl.ds(pl.multiple_of(row * heads, heads), heads)
                            o_buf[c, place, :] = mixed[:, c * LANES : (c + 1) * LANES]

        @pl.when(group + SLOTS < groups)
        def _():
            start(group + SLOTS, slot)

        return carry

    lax.fori_loop(0, groups, step, 0)
    for h in range(heads):
        for c in range(latent // LANES):
            place = pl.ds(h * latent + c * LANES, LANES)
            o_ref[:, place] = o_buf[c, pl.ds(h, rows, stride=heads), :].astype(jnp.bfloat16)


def attention(layer, q, lengths, cache_t, rows, latent):
    heads = q.shape[1] // rows
    kv_dim, seq_len = cache_t.shape[2:]
    scale = (3 * (kv_dim - latent)) ** -0.5
    return pl.pallas_call(
        functools.partial(attention_kernel, layer, scale),
        out_shape=jax.ShapeDtypeStruct((rows, heads * latent), jnp.bfloat16),
        in_specs=[
            pl.BlockSpec(memory_space=pltpu.SMEM),
            pl.BlockSpec(memory_space=pltpu.VMEM),
            pl.BlockSpec(memory_space=pl.ANY),
        ],
        out_specs=pl.BlockSpec(memory_space=pltpu.VMEM),
        scratch_shapes=[
            pltpu.VMEM((SLOTS, SEQS, kv_dim, seq_len), jnp.bfloat16),
            pltpu.VMEM((SEQS * heads, seq_len), jnp.float32),
            pltpu.VMEM((SEQS * heads, seq_len), jnp.bfloat16),
            pltpu.VMEM((latent // LANES, rows * heads, LANES), jnp.float32),
            pltpu.SemaphoreType.DMA((SLOTS,)),
        ],
        compiler_params=pltpu.CompilerParams(vmem_limit_bytes=40 * MIB),
        name=f'attention_{layer}',
    )(lengths, q, cache_t)


def tail_kernel(layer, next_q, *refs):
    refs = list(refs)

    def take(count):
        taken, refs[:count] = refs[:count], []
        return taken

    o_hbm, x_hbm, gain_hbm, wo_hbm, wg_hbm, wu_hbm, wd_hbm = take(7)
    if next_q:
        q_gain_hbm, wq_hbm = take(2)
    (out_ref,) = take(1)
    if next_q:
        (q_ref,) = take(1)
    o_all, x_old, wg, wu, wd, x_mid, g_all, a_all, p_other, p_own, part_in, cross_in, own_in, gain_ref = take(14)
    in_sem, wo_sem, w_sem, wd_sem = take(4)
    o_send, o_recv, xo_send, xo_recv, xp_send, xp_recv, xc_send, xc_recv, xf_send, xf_recv = take(10)
    p1_send, p1_recv, p2_send, p2_recv, p3_send, p3_recv = take(6)
    if next_q:
        wq, q_send, x_in, q_gain_ref, wq_sem, x_send, x_recv, q_ssem, q_rsem = take(9)

    rows, d_model = x_hbm.shape
    chip_rows = 2 * rows
    half = d_model // 2
    hidden = wd_hbm.shape[1]
    o_width = o_hbm.shape[1]
    o_part = o_width // O_PARTS
    x_pieces = half // COLS
    out_pieces = d_model // COLS
    steps = [(start, min(HID, hidden - start)) for start in range(0, hidden, HID)]

    me = lax.axis_index('dp')
    core = lax.rem(me, 2)
    partner = me + 1 - 2 * core
    across = lax.rem(me + 2, 4)
    other_core = 1 - core
    my_rows = pl.ds(pl.multiple_of(core * rows, rows), rows)
    partner_rows = pl.ds(pl.multiple_of(other_core * rows, rows), rows)

    def wo_place(j, k):
        region = wg if j < x_pieces // 2 else wu
        lane = (j % (x_pieces // 2)) * O_PARTS * COLS + k * COLS
        return region.at[pl.ds(0, o_part), pl.ds(lane, COLS)]

    def wo_copy(j, k):
        columns = pl.ds(pl.multiple_of(core * half + j * COLS, COLS), COLS)
        return pltpu.make_async_copy(
            wo_hbm.at[layer, pl.ds(k * o_part, o_part), columns], wo_place(j, k), wo_sem.at[j, k]
        )

    def gate_copy(i):
        window = pl.ds(*steps[i])
        return pltpu.make_async_copy(wg_hbm.at[layer, window], wg.at[window], w_sem.at[0, i])

    def up_copy(i):
        window = pl.ds(*steps[i])
        return pltpu.make_async_copy(wu_hbm.at[layer, window], wu.at[window], w_sem.at[1, i])

    def down_copy(n):
        columns = pl.ds(n * DOWN, DOWN)
        return pltpu.make_async_copy(wd_hbm.at[layer, :, columns], wd.at[n], wd_sem.at[n])

    o_parts = [pl.ds(k * o_part, o_part) for k in range(O_PARTS)]
    o_own = [pltpu.make_async_copy(o_hbm.at[:, w], o_all.at[my_rows, w], in_sem.at[k]) for k, w in enumerate(o_parts)]
    x_own = pltpu.make_async_copy(
        x_hbm.at[:, pl.ds(pl.multiple_of(core * half, half), half)], x_old.at[my_rows], in_sem.at[O_PARTS]
    )
    gains = [pltpu.make_async_copy(gain_hbm, gain_ref, in_sem.at[O_PARTS + 1])]
    if next_q:
        gains.append(pltpu.make_async_copy(q_gain_hbm, q_gain_ref, in_sem.at[O_PARTS + 2]))
    for c in o_own + [x_own] + gains:
        c.start()
    for j in range(x_pieces):
        for k in range(O_PARTS):
            wo_copy(j, k).start(priority=BULK)

    enter(partner, across)

    o_out = [remote_copy(o_hbm.at[:, w], o_all.at[my_rows, w], o_send.at[k], o_recv.at[k], partner) for k, w in enumerate(o_parts)]
    x_out = remote_copy(
        x_hbm.at[:, pl.ds(pl.multiple_of(other_core * half, half), half)], x_old.at[my_rows], xo_send, xo_recv, partner
    )
    for c in o_out:
        c.start()
    x_out.start()

    def to_partner(j):
        piece = x_mid.at[core, pl.ds(0, chip_rows), pl.ds(j * COLS, COLS)]
        return remote_copy(piece, piece, xp_send.at[j], xp_recv.at[j], partner)

    def to_across(j):
        src = x_mid.at[core, pl.ds(0, chip_rows), pl.ds(j * COLS, COLS)]
        dst = x_mid.at[core, pl.ds(chip_rows, chip_rows), pl.ds(j * COLS, COLS)]
        return remote_copy(src, dst, xc_send.at[j], xc_recv.at[j], across)

    def forward(j):
        piece = x_mid.at[core, pl.ds(chip_rows, chip_rows), pl.ds(j * COLS, COLS)]
        return remote_copy(piece, piece, xf_send.at[j], xf_recv.at[j], partner)

    for j in range(x_pieces):
        product = None
        for k in range(O_PARTS):
            if j == 0:
                o_own[k].wait()
                o_out[k].wait_recv()
            wo_copy(j, k).wait()
            term = jnp.dot(o_all[:, o_parts[k]], wo_place(j, k)[...], preferred_element_type=jnp.float32)
            product = term if product is None else product + term
        if j == 0:
            x_own.wait()
            x_out.wait_recv()
            for c in gains:
                c.wait()
        columns = pl.ds(j * COLS, COLS)
        x_mid[core, pl.ds(0, chip_rows), columns] = (x_old[:, columns].astype(jnp.float32) + product).astype(jnp.bfloat16)
        to_across(j).start()
        to_partner(j).start()
        if j == 0:
            for n in range(d_model // DOWN):
                down_copy(n).start(priority=BULK)
        if j == x_pieces // 2 - 1:
            for i in range(len(steps)):
                gate_copy(i).start(priority=BULK)
        if j == x_pieces - 1:
            for i in range(len(steps)):
                up_copy(i).start(priority=BULK)

    if next_q:
        q_width = wq.shape[2]
        q_pairs = q_ssem.shape[0]
        q_places = [wq.at[0], wq.at[1]] + [w.at[pl.ds(0, d_model), pl.ds(0, q_width)] for w in (wg, wu)]

        def wq_copy(p):
            columns = pl.ds(pl.multiple_of((core * q_pairs + p) * q_width, 128), q_width)
            return pltpu.make_async_copy(wq_hbm.at[layer + 1, :, columns], q_places[p], wq_sem.at[p])

        wq_copy(0).start(priority=BULK)
        wq_copy(1).start(priority=BULK)

    def normalize(start):
        window = pl.ds(start, chip_rows)
        halves = [x_mid[h, window, :].astype(jnp.float32) for h in range(2)]
        total = sum(jnp.sum(v * v, axis=-1, keepdims=True) for v in halves)
        factor = lax.rsqrt(total * (1.0 / d_model) + NORM_EPS)
        for h in range(2):
            gain = gain_ref[pl.ds(layer, 1), pl.ds(h * half, half)]
            g_all[window, pl.ds(h * half, half)] = (halves[h] * factor * gain).astype(jnp.bfloat16)

    for j in range(x_pieces):
        to_partner(j).wait_recv()
    normalize(0)
    for j in range(x_pieces):
        to_across(j).wait_recv()
        forward(j).start()
    for j in range(x_pieces):
        forward(j).wait_recv()
    normalize(chip_rows)

    for i, step in enumerate(steps):
        gate_copy(i).wait()
        up_copy(i).wait()
        window = pl.ds(*step)
        dims = (((1,), (1,)), ((), ()))
        gate = lax.dot_general(g_all[...], wg[window, :], dims, preferred_element_type=jnp.float32)
        up = lax.dot_general(g_all[...], wu[window, :], dims, preferred_element_type=jnp.float32)
        a_all[:, window] = (jax.nn.silu(gate) * up).astype(jnp.bfloat16)

    if next_q:
        wq_copy(2).start(priority=BULK)
        wq_copy(3).start(priority=BULK)

    def pair_other(n):
        return remote_copy(p_other.at[n, partner_rows], part_in.at[n], p1_send.at[n], p1_recv.at[n], partner)

    def cross(n):
        return remote_copy(part_in.at[n], cross_in.at[n], p2_send.at[n], p2_recv.at[n], across)

    def pair_own(n):
        return remote_copy(p_own.at[n, partner_rows], own_in.at[n], p3_send.at[n], p3_recv.at[n], partner)

    def send_sum(n):
        pair_other(n).wait_recv()
        part_in[n] = p_other[n, my_rows] + part_in[n]
        cross(n).start()

    per_step = DOWN // COLS
    down_steps = d_model // DOWN
    for d in range(down_steps):
        down_copy(d).wait()
    for d in range(down_steps):
        product = jnp.dot(a_all[pl.ds(chip_rows, chip_rows), :], wd[d], preferred_element_type=jnp.float32)
        for e in range(per_step):
            n = d * per_step + e
            p_other[n] = product[:, e * COLS : (e + 1) * COLS]
            pair_other(n).start()
        if d >= 2:
            for e in range(per_step):
                send_sum((d - 2) * per_step + e)
    for d in range(down_steps):
        if d < 2:
            for e in range(per_step):
                send_sum((d + down_steps - 2) * per_step + e)
        product = jnp.dot(a_all[pl.ds(0, chip_rows), :], wd[d], preferred_element_type=jnp.float32)
        for e in range(per_step):
            n = d * per_step + e
            p_own[n] = product[:, e * COLS : (e + 1) * COLS]
            pair_own(n).start()

    def next_x(n):
        piece = pl.ds(n * COLS, COLS)
        return remote_copy(out_ref.at[:, piece], x_in.at[:, piece], x_send.at[n], x_recv.at[n], partner)

    per_half = half // COLS
    for n in range(out_pieces):
        pair_own(n).wait_recv()
        cross(n).wait_recv()
        h, columns = n // per_half, pl.ds((n % per_half) * COLS, COLS)
        total = (p_own[n, my_rows] + own_in[n]) + cross_in[n]
        out_ref[:, pl.ds(n * COLS, COLS)] = (x_mid[h, my_rows, columns].astype(jnp.float32) + total).astype(jnp.bfloat16)
        if next_q:
            next_x(n).start()

    if next_q:
        gain = q_gain_ref[pl.ds(layer + 1, 1), :]
        g_all[pl.ds(0, rows), :] = rms_scaled(out_ref[...], gain)
        for n in range(out_pieces):
            next_x(n).wait_recv()
        g_all[pl.ds(rows, rows), :] = rms_scaled(x_in[...], gain)
        weights = [(wq_copy(p).wait, q_places[p]) for p in range(q_pairs)]
        gives = project_q(
            g_all.at[pl.ds(0, chip_rows)], weights, core, partner, q_ref, q_send, q_ssem, q_rsem
        )

    for c in o_out:
        c.wait_send()
    x_out.wait_send()
    for j in range(x_pieces):
        to_partner(j).wait_send()
        to_across(j).wait_send()
        forward(j).wait_send()
    for n in range(out_pieces):
        pair_other(n).wait_send()
        cross(n).wait_send()
        pair_own(n).wait_send()
    if next_q:
        for n in range(out_pieces):
            next_x(n).wait_send()
        for give in gives:
            give.wait()


def tail(layer, o, x, gain, wo, wg_t, wu_t, wd, next_q):
    rows, d_model = x.shape
    hidden = wd.shape[1]
    width = o.shape[1]
    half = d_model // 2
    x_pieces, out_pieces, down_steps = half // COLS, d_model // COLS, d_model // DOWN
    steps = -(-hidden // HID)
    dma = pltpu.SemaphoreType.DMA
    any_space = pl.BlockSpec(memory_space=pl.ANY)
    vmem = pl.BlockSpec(memory_space=pltpu.VMEM)
    in_specs = [any_space, any_space, any_space, any_space, any_space, any_space, any_space]
    out_shape = [jax.ShapeDtypeStruct((rows, d_model), jnp.bfloat16)]
    piece = pltpu.VMEM((out_pieces, rows, COLS), jnp.float32)
    scratch = [
        pltpu.VMEM((2 * rows, width), jnp.bfloat16),
        pltpu.VMEM((2 * rows, half), jnp.bfloat16),
        pltpu.VMEM((hidden, d_model), jnp.bfloat16),
        pltpu.VMEM((hidden, d_model), jnp.bfloat16),
        pltpu.VMEM((down_steps, hidden, DOWN), jnp.bfloat16),
        pltpu.VMEM((2, 4 * rows, half), jnp.bfloat16),
        pltpu.VMEM((4 * rows, d_model), jnp.bfloat16),
        pltpu.VMEM((4 * rows, hidden), jnp.bfloat16),
        pltpu.VMEM((out_pieces, 2 * rows, COLS), jnp.float32),
        pltpu.VMEM((out_pieces, 2 * rows, COLS), jnp.float32),
        piece, piece, piece, pltpu.VMEM(gain.shape, jnp.float32),
        dma((O_PARTS + 3,)), dma((x_pieces, O_PARTS)), dma((2, steps)), dma((down_steps,)),
        dma((O_PARTS,)), dma((O_PARTS,)), dma, dma,
        dma((x_pieces,)), dma((x_pieces,)), dma((x_pieces,)), dma((x_pieces,)), dma((x_pieces,)), dma((x_pieces,)),
        dma((out_pieces,)), dma((out_pieces,)), dma((out_pieces,)), dma((out_pieces,)), dma((out_pieces,)), dma((out_pieces,)),
    ]
    operands = [o, x, gain, wo, wg_t, wu_t, wd]
    if next_q is not None:
        q_gain, wq, heads = next_q
        kv_dim, pairs = wq.shape[2] // heads, heads // 4
        operands += [q_gain, wq]
        in_specs += [any_space, any_space]
        out_shape.append(jax.ShapeDtypeStruct((-(-kv_dim // LANES), heads * rows, LANES), jnp.float32))
        scratch += [
            pltpu.VMEM((2, d_model, 2 * kv_dim), jnp.bfloat16),
            pltpu.VMEM((pairs, -(-kv_dim // LANES), 2 * rows, LANES), jnp.float32),
            pltpu.VMEM((rows, d_model), jnp.bfloat16),
            pltpu.VMEM(q_gain.shape, jnp.float32),
            dma((pairs,)), dma((out_pieces,)), dma((out_pieces,)), dma((pairs,)), dma((pairs,)),
        ]
    return pl.pallas_call(
        functools.partial(tail_kernel, layer, next_q is not None),
        out_shape=out_shape,
        in_specs=in_specs,
        out_specs=[vmem] * len(out_shape),
        scratch_shapes=scratch,
        compiler_params=pltpu.CompilerParams(collective_id=layer, has_side_effects=True, vmem_limit_bytes=59 * MIB),
        name=f'tail_{layer}',
    )(*operands)


def solution(mesh):
    row_axes = ('replica', 'dp')

    def local_step(x_rows, len_rows, cache, attn_gain, ffn_gain, w_query, w_attn_out, w_up, w_gate, w_down):
        layers, rows, _, kv_dim = cache.shape
        heads = w_query.shape[2] // kv_dim
        latent = w_attn_out.shape[1] // heads
        cache_t = jnp.swapaxes(cache, 2, 3)
        up_t, gate_t = jnp.swapaxes(w_up, 1, 2), jnp.swapaxes(w_gate, 1, 2)
        q = head(x_rows, attn_gain, w_query, heads)
        for layer in range(layers):
            mixed = attention(layer, q, len_rows, cache_t, rows, latent)
            next_q = (attn_gain, w_query, heads) if layer + 1 < layers else None
            outs = tail(layer, mixed, x_rows, ffn_gain, w_attn_out, gate_t, up_t, w_down, next_q)
            x_rows, q = outs[0], outs[-1]
        return x_rows

    return jax.shard_map(
        local_step,
        mesh=mesh,
        in_specs=(P(row_axes, None), P(row_axes), P(None, row_axes, None, None), P(), P(), P(), P(),
                  P(None, None, 'dp'), P(None, None, 'dp'), P(None, 'dp', None)),
        out_specs=P(row_axes, None),
        check_vma=False,
    )
```

```python
import functools

import jax
import jax.numpy as jnp
from jax import lax
from jax.experimental import pallas as pl
from jax.experimental.pallas import tpu as pltpu
from jax.sharding import PartitionSpec as P

NORM_EPS = 1e-6
MESH = pl.DeviceIdType.MESH
SEQS = 8
SLOTS = 3
TBLK = 128
PARTS = 2
COLS = 256
HID = 512
SUPER = 1280
DOWN = 512
O_PARTS = 4
MIB = 1024 * 1024
LANES = 128
BULK = 1


def remote_copy(src, dst, send, recv, device):
    return pltpu.make_async_remote_copy(
        src_ref=src, dst_ref=dst, send_sem=send, recv_sem=recv, device_id={'dp': device}, device_id_type=MESH
    )


def enter(*peers):
    barrier = pltpu.get_barrier_semaphore()
    for peer in peers:
        pl.semaphore_signal(barrier, inc=1, device_id={'dp': peer}, device_id_type=MESH)
    pl.semaphore_wait(barrier, len(peers))


def hidden_steps(hidden):
    ends = [min(start + SUPER, hidden) for start in range(0, hidden, SUPER)]
    return [(at, min(HID, end - at)) for t, end in enumerate(ends) for at in range(t * SUPER, end, HID)]


def rms_scaled(rows, gain):
    rows_f = rows.astype(jnp.float32)
    mean_sq = jnp.mean(rows_f * rows_f, axis=-1, keepdims=True)
    return (rows_f * lax.rsqrt(mean_sq + NORM_EPS) * gain).astype(jnp.bfloat16)


def project_pair(p, h_ref, parts, core, pairs, kv_dim, partner, q_ref, q_send, send_sem, recv_sem):
    rows = q_send.shape[2] // 2
    q = [jnp.dot(h_ref[...], part[...], preferred_element_type=jnp.float32) for part in parts]
    q = q[0] if len(q) == 1 else jnp.concatenate(q, axis=1)
    q = q.astype(jnp.bfloat16).astype(jnp.float32)
    for e in range(2):
        own = pl.ds(pl.multiple_of((core * pairs + p) * 2 * rows + e * rows, rows), rows)
        for c in range(q_ref.shape[0]):
            size = min(LANES, kv_dim - c * LANES)
            part = q[:, e * kv_dim + c * LANES :][:, :size]
            q_ref[c, own, pl.ds(0, size)] = part[:rows]
            q_send[p, c, pl.ds(e * rows, rows), pl.ds(0, size)] = part[rows:]
    give_pair(p, core, pairs, partner, q_ref, q_send, send_sem, recv_sem).start()


def give_pair(p, core, pairs, partner, q_ref, q_send, send_sem, recv_sem):
    size = q_send.shape[2]
    heads = pl.ds(pl.multiple_of((core * pairs + p) * size, size), size)
    return remote_copy(q_send.at[p], q_ref.at[:, heads], send_sem.at[p], recv_sem.at[p], partner)


def head_kernel(x_hbm, gain_hbm, wq_hbm, q_ref, x_ref, gain_ref, x_in, h_ref, wq, q_send, in_sem, wq_sem, x_send, x_recv, q_ssem, q_rsem):
    rows = x_hbm.shape[0]
    width = wq.shape[2]
    pairs = wq.shape[0]
    me = lax.axis_index('dp')
    core = lax.rem(me, 2)
    partner = me + 1 - 2 * core

    def wq_copy(p):
        columns = pl.ds(pl.multiple_of((core * pairs + p) * width, 128), width)
        return pltpu.make_async_copy(wq_hbm.at[0, :, columns], wq.at[p], wq_sem.at[p])

    x_own = pltpu.make_async_copy(x_hbm, x_ref, in_sem.at[0])
    gain_own = pltpu.make_async_copy(gain_hbm, gain_ref, in_sem.at[1])
    x_own.start()
    gain_own.start()
    for p in range(pairs):
        wq_copy(p).start(priority=BULK)
    x_own.wait()
    gain_own.wait()
    enter(partner)
    swap = remote_copy(x_ref, x_in, x_send, x_recv, partner)
    swap.start()
    h_ref[pl.ds(0, rows), :] = rms_scaled(x_ref[...], gain_ref[pl.ds(0, 1), :])
    swap.wait_recv()
    h_ref[pl.ds(rows, rows), :] = rms_scaled(x_in[...], gain_ref[pl.ds(0, 1), :])

    @pl.loop(0, pairs)
    def _(p):
        wq_copy(p).wait()
        project_pair(p, h_ref, [wq.at[p]], core, pairs, width // 2, partner, q_ref, q_send, q_ssem, q_rsem)

    swap.wait_send()
    for p in range(pairs):
        give_pair(p, core, pairs, partner, q_ref, q_send, q_ssem, q_rsem).wait()


def head(x, gain, wq, heads):
    rows, d_model = x.shape
    kv_dim = wq.shape[2] // heads
    pairs = heads // 4
    dma = pltpu.SemaphoreType.DMA
    vmem = pl.BlockSpec(memory_space=pltpu.VMEM)
    return pl.pallas_call(
        head_kernel,
        out_shape=jax.ShapeDtypeStruct((-(-kv_dim // LANES), heads * rows, LANES), jnp.float32),
        in_specs=[pl.BlockSpec(memory_space=pltpu.HBM)] * 3,
        out_specs=vmem,
        scratch_shapes=[
            pltpu.VMEM((rows, d_model), jnp.bfloat16),
            pltpu.VMEM(gain.shape, jnp.float32),
            pltpu.VMEM((rows, d_model), jnp.bfloat16),
            pltpu.VMEM((2 * rows, d_model), jnp.bfloat16),
            pltpu.VMEM((pairs, d_model, 2 * kv_dim), jnp.bfloat16),
            pltpu.VMEM((pairs, -(-kv_dim // LANES), 2 * rows, LANES), jnp.float32),
            dma((2,)), dma((pairs,)), dma, dma, dma((pairs,)), dma((pairs,)),
        ],
        compiler_params=pltpu.CompilerParams(collective_id=7, has_side_effects=True, vmem_limit_bytes=48 * MIB),
        name='head',
    )(x, gain, wq)


def attention_kernel(layer, scale, len_ref, q_ref, cache_ref, o_ref, buf, score_buf, prob_buf, o_buf, sem):
    rows = o_ref.shape[0]
    heads = q_ref.shape[1] // rows
    kv_dim, seq_len = cache_ref.shape[2:]
    latent = o_ref.shape[1] // heads
    groups = rows // SEQS
    max_blocks = seq_len // TBLK

    def blocks_of(group):
        longest = len_ref[group * SEQS]
        for i in range(1, SEQS):
            longest = jnp.maximum(longest, len_ref[group * SEQS + i])
        return lax.div(longest + (TBLK - 1), TBLK)

    def copy(group, slot, n):
        return pltpu.make_async_copy(
            cache_ref.at[layer, pl.ds(group * SEQS, SEQS), :, pl.ds(0, n * TBLK)],
            buf.at[slot, :, :, pl.ds(0, n * TBLK)],
            sem.at[slot],
        )

    def start(group, slot):
        blocks = blocks_of(group)
        for n in range(1, max_blocks + 1):

            @pl.when(blocks == n)
            def _():
                copy(group, slot, n).start()

    for group in range(min(SLOTS, groups)):
        start(group, group)

    def step(group, carry):
        slot = lax.rem(group, SLOTS)
        blocks = blocks_of(group)
        for n in range(1, max_blocks + 1):

            @pl.when(blocks == n)
            def _():
                copy(group, slot, n).wait()
                width = n * TBLK
                positions = lax.broadcasted_iota(jnp.int32, (heads, width), 1)
                for i in range(SEQS):
                    row = group * SEQS + i
                    query = [q_ref[c, pl.ds(row, heads, stride=rows), :] for c in range(q_ref.shape[0])]
                    query = jnp.concatenate(query, axis=1)[:, :kv_dim].astype(jnp.bfloat16)
                    score_buf[pl.ds(i * heads, heads), pl.ds(0, width)] = jnp.dot(
                        query, buf[slot, i, :, pl.ds(0, width)], preferred_element_type=jnp.float32
                    )
                for part in range(PARTS):
                    size = SEQS // PARTS
                    for i in range(part * size, (part + 1) * size):
                        row = group * SEQS + i
                        scores = score_buf[pl.ds(i * heads, heads), pl.ds(0, width)]
                        scores = jnp.where(positions < len_ref[row], scores * scale, -jnp.inf)
                        top = jnp.max(scores, axis=-1, keepdims=True)
                        probs = jnp.exp(scores - top)
                        probs = probs * (1.0 / jnp.sum(probs, axis=-1, keepdims=True))
                        prob_buf[pl.ds(i * heads, heads), pl.ds(0, width)] = probs.astype(jnp.bfloat16)
                    for i in range(part * size, (part + 1) * size):
                        row = group * SEQS + i
                        mixed = lax.dot_general(
                            prob_buf[pl.ds(i * heads, heads), pl.ds(0, width)],
                            buf[slot, i, pl.ds(0, latent), pl.ds(0, width)],
                            (((1,), (1,)), ((), ())),
                            preferred_element_type=jnp.float32,
                        )
                        for c in range(latent // LANES):
                            place = pl.ds(pl.multiple_of(row * heads, heads), heads)
                            o_buf[c, place, :] = mixed[:, c * LANES : (c + 1) * LANES]

        @pl.when(group + SLOTS < groups)
        def _():
            start(group + SLOTS, slot)

        return carry

    lax.fori_loop(0, groups, step, 0)
    for h in range(heads):
        for c in range(latent // LANES):
            place = pl.ds(h * latent + c * LANES, LANES)
            o_ref[:, place] = o_buf[c, pl.ds(h, rows, stride=heads), :].astype(jnp.bfloat16)


def attention(layer, q, lengths, cache_t, rows, latent):
    heads = q.shape[1] // rows
    kv_dim, seq_len = cache_t.shape[2:]
    scale = (3 * (kv_dim - latent)) ** -0.5
    return pl.pallas_call(
        functools.partial(attention_kernel, layer, scale),
        out_shape=jax.ShapeDtypeStruct((rows, heads * latent), jnp.bfloat16),
        in_specs=[
            pl.BlockSpec(memory_space=pltpu.SMEM),
            pl.BlockSpec(memory_space=pltpu.VMEM),
            pl.BlockSpec(memory_space=pl.ANY),
        ],
        out_specs=pl.BlockSpec(memory_space=pltpu.VMEM),
        scratch_shapes=[
            pltpu.VMEM((SLOTS, SEQS, kv_dim, seq_len), jnp.bfloat16),
            pltpu.VMEM((SEQS * heads, seq_len), jnp.float32),
            pltpu.VMEM((SEQS * heads, seq_len), jnp.bfloat16),
            pltpu.VMEM((latent // LANES, rows * heads, LANES), jnp.float32),
            pltpu.SemaphoreType.DMA((SLOTS,)),
        ],
        compiler_params=pltpu.CompilerParams(vmem_limit_bytes=40 * MIB),
        name=f'attention_{layer}',
    )(lengths, q, cache_t)


def tail_kernel(layer, next_q, *refs):
    refs = list(refs)

    def take(count):
        taken, refs[:count] = refs[:count], []
        return taken

    o_ref, x_hbm, gain_hbm, wo_ref, wg_hbm, wu_hbm, wd_hbm = take(7)
    if next_q:
        q_gain_hbm, wq_hbm = take(2)
    (out_ref,) = take(1)
    if next_q:
        (q_ref,) = take(1)
    o_all, x_old, wgu, wd, x_mid, g_all, a_all, p_other, p_own, part_in, cross_in, own_in, gain_ref = take(13)
    in_sem, wo_sem, w_sem, wd_sem = take(4)
    o_send, o_recv, xo_send, xo_recv, xp_send, xp_recv, xc_send, xc_recv, xf_send, xf_recv = take(10)
    p1_send, p1_recv, p2_send, p2_recv, p3_send, p3_recv = take(6)
    if next_q:
        wq, q_send, x_in, q_gain_ref, wq_sem, x_send, x_recv, q_ssem, q_rsem = take(9)

    rows, d_model = x_hbm.shape
    chip_rows = 2 * rows
    half = d_model // 2
    hidden = wd_hbm.shape[1]
    o_width = o_ref.shape[1]
    o_part = o_width // O_PARTS
    x_pieces = half // COLS
    out_pieces = d_model // COLS
    steps = hidden_steps(hidden)
    loop_steps = -(-SUPER // HID)
    loops = hidden // SUPER

    me = lax.axis_index('dp')
    core = lax.rem(me, 2)
    partner = me + 1 - 2 * core
    across = lax.rem(me + 2, 4)
    other_core = 1 - core
    my_rows = pl.ds(pl.multiple_of(core * rows, rows), rows)
    partner_rows = pl.ds(pl.multiple_of(other_core * rows, rows), rows)

    wg, wu = wgu.at[0], wgu.at[1]
    per_region = x_pieces // 2

    def wo_place(j, k):
        lane = pl.multiple_of(lax.rem(j, per_region) * (O_PARTS * COLS) + k * COLS, COLS)
        return wgu.at[lax.div(j, per_region), pl.ds(0, o_part), pl.ds(lane, COLS)]

    def wo_copy(j, k):
        columns = pl.ds(pl.multiple_of(core * half + j * COLS, COLS), COLS)
        return pltpu.make_async_copy(
            wo_ref.at[layer, pl.ds(k * o_part, o_part), columns], wo_place(j, k), wo_sem.at[j, k]
        )

    def gate_copy(i):
        window = pl.ds(*steps[i])
        return pltpu.make_async_copy(wg_hbm.at[layer, window], wg.at[window], w_sem.at[0, i])

    def up_copy(i):
        window = pl.ds(*steps[i])
        return pltpu.make_async_copy(wu_hbm.at[layer, window], wu.at[window], w_sem.at[1, i])

    def down_copy(n):
        columns = pl.ds(n * DOWN, DOWN)
        return pltpu.make_async_copy(wd_hbm.at[layer, :, columns], wd.at[n], wd_sem.at[n])

    o_parts = [pl.ds(k * o_part, o_part) for k in range(O_PARTS)]
    o_own = [pltpu.make_async_copy(o_ref.at[:, w], o_all.at[my_rows, w], in_sem.at[k]) for k, w in enumerate(o_parts)]
    x_own = pltpu.make_async_copy(
        x_hbm.at[:, pl.ds(pl.multiple_of(core * half, half), half)], x_old.at[my_rows], in_sem.at[O_PARTS]
    )
    gains = [pltpu.make_async_copy(gain_hbm, gain_ref, in_sem.at[O_PARTS + 1])]
    if next_q:
        gains.append(pltpu.make_async_copy(q_gain_hbm, q_gain_ref, in_sem.at[O_PARTS + 2]))
    for c in o_own + [x_own] + gains:
        c.start()
    for j in range(x_pieces):
        for k in range(O_PARTS):
            wo_copy(j, k).start(priority=BULK)

    enter(partner, across)

    o_out = [remote_copy(o_ref.at[:, w], o_all.at[my_rows, w], o_send.at[k], o_recv.at[k], partner) for k, w in enumerate(o_parts)]
    x_out = remote_copy(
        x_hbm.at[:, pl.ds(pl.multiple_of(other_core * half, half), half)], x_old.at[my_rows], xo_send, xo_recv, partner
    )
    for c in o_out:
        c.start()
    x_out.start()

    def piece_of(j):
        return pl.ds(pl.multiple_of(j * COLS, COLS), COLS)

    def to_partner(j):
        piece = x_mid.at[core, pl.ds(0, chip_rows), piece_of(j)]
        return remote_copy(piece, piece, xp_send.at[j], xp_recv.at[j], partner)

    def to_across(j):
        src = x_mid.at[core, pl.ds(0, chip_rows), piece_of(j)]
        dst = x_mid.at[core, pl.ds(chip_rows, chip_rows), piece_of(j)]
        return remote_copy(src, dst, xc_send.at[j], xc_recv.at[j], across)

    def forward(j):
        piece = x_mid.at[core, pl.ds(chip_rows, chip_rows), pl.ds(j * COLS, COLS)]
        return remote_copy(piece, piece, xf_send.at[j], xf_recv.at[j], partner)

    for c in [x_own] + gains + o_own:
        c.wait()
    for c in [x_out] + o_out:
        c.wait_recv()

    @pl.loop(0, x_pieces)
    def _(j):
        for k in range(O_PARTS):
            wo_copy(j, k).wait()
        terms = [
            jnp.dot(o_all[:, o_parts[k]], wo_place(j, k)[...], preferred_element_type=jnp.float32) for k in range(O_PARTS)
        ]
        product = functools.reduce(jnp.add, terms)
        columns = piece_of(j)
        x_mid[core, pl.ds(0, chip_rows), columns] = (x_old[:, columns].astype(jnp.float32) + product).astype(jnp.bfloat16)
        to_across(j).start()
        to_partner(j).start()

        for at in range(2):

            @pl.when(j == at * per_region)
            def _():
                down_copy(at).start(priority=BULK)

            @pl.when(j == (at + 1) * per_region - 1)
            def _():
                for i in range(len(steps)):
                    (gate_copy, up_copy)[at](i).start(priority=BULK)

    for n in range(2, d_model // DOWN):
        down_copy(n).start(priority=BULK)

    if next_q:
        q_pairs = q_ssem.shape[0]
        q_width = wq_hbm.shape[2] // (2 * q_pairs)
        spare = d_model - q_width
        over = q_width - spare

        def wq_parts(p):
            region = (wg, wu)[p % 2]
            spans = [(region, 0, 0, q_width)] if p < 2 else [(region, q_width, 0, spare), (wq, (p % 2) * over, spare, over)]
            places, copies = [], []
            for i, (buffer, lane, offset, size) in enumerate(spans):
                columns = pl.ds(pl.multiple_of((core * q_pairs + p) * q_width + offset, LANES), size)
                places.append(buffer.at[pl.ds(0, d_model), pl.ds(lane, size)])
                copies.append(pltpu.make_async_copy(wq_hbm.at[layer + 1, :, columns], places[-1], wq_sem.at[p, i]))
            return places, copies

    def normalize(start):
        window = pl.ds(start, chip_rows)
        halves = [x_mid[h, window, :].astype(jnp.float32) for h in range(2)]
        total = sum(jnp.sum(v * v, axis=-1, keepdims=True) for v in halves)
        factor = lax.rsqrt(total * (1.0 / d_model) + NORM_EPS)
        for h in range(2):
            gain = gain_ref[pl.ds(layer, 1), pl.ds(h * half, half)]
            g_all[window, pl.ds(h * half, half)] = (halves[h] * factor * gain).astype(jnp.bfloat16)

    for j in range(x_pieces):
        to_partner(j).wait_recv()
    normalize(0)
    for j in range(x_pieces):
        to_across(j).wait_recv()
        forward(j).start()
    for j in range(x_pieces):
        forward(j).wait_recv()
    normalize(chip_rows)

    def gate_up(i, start, size):
        window = pl.ds(start, size)
        pltpu.make_async_copy(wg_hbm.at[layer, window], wg.at[window], w_sem.at[0, i]).wait()
        pltpu.make_async_copy(wu_hbm.at[layer, window], wu.at[window], w_sem.at[1, i]).wait()
        dims = (((1,), (1,)), ((), ()))
        gate = lax.dot_general(g_all[...], wg[window, :], dims, preferred_element_type=jnp.float32)
        up = lax.dot_general(g_all[...], wu[window, :], dims, preferred_element_type=jnp.float32)
        a_all[:, window] = (jax.nn.silu(gate) * up).astype(jnp.bfloat16)

    @pl.loop(0, loops)
    def _(t):
        for i in range(loop_steps):
            start, size = steps[i]
            gate_up(t * loop_steps + i, pl.multiple_of(t * SUPER + start, LANES), size)

    for i in range(loops * loop_steps, len(steps)):
        gate_up(i, *steps[i])

    if next_q:
        for p in range(q_pairs):
            for c in wq_parts(p)[1]:
                c.start(priority=BULK)

    def pair_other(n):
        return remote_copy(p_other.at[n, partner_rows], part_in.at[n], p1_send.at[n], p1_recv.at[n], partner)

    def cross(n):
        return remote_copy(part_in.at[n], cross_in.at[n], p2_send.at[n], p2_recv.at[n], across)

    def pair_own(n):
        return remote_copy(p_own.at[n, partner_rows], own_in.at[n], p3_send.at[n], p3_recv.at[n], partner)

    def send_sum(n):
        pair_other(n).wait_recv()
        part_in[n] = p_other[n, my_rows] + part_in[n]
        cross(n).start()

    per_step = DOWN // COLS
    down_steps = d_model // DOWN
    for d in range(down_steps):
        down_copy(d).wait()
    for d in range(down_steps):
        product = jnp.dot(a_all[pl.ds(chip_rows, chip_rows), :], wd[d], preferred_element_type=jnp.float32)
        for e in range(per_step):
            n = d * per_step + e
            p_other[n] = product[:, e * COLS : (e + 1) * COLS]
            pair_other(n).start()
        if d >= 2:
            for e in range(per_step):
                send_sum((d - 2) * per_step + e)
    @pl.loop(0, down_steps)
    def _(d):
        @pl.when(d < 2)
        def _():
            for e in range(per_step):
                send_sum((d + down_steps - 2) * per_step + e)

        product = jnp.dot(a_all[pl.ds(0, chip_rows), :], wd[d], preferred_element_type=jnp.float32)
        for e in range(per_step):
            n = d * per_step + e
            p_own[n] = product[:, e * COLS : (e + 1) * COLS]
            pair_own(n).start()

    def next_x(n):
        piece = pl.ds(n * COLS, COLS)
        return remote_copy(out_ref.at[:, piece], x_in.at[:, piece], x_send.at[n], x_recv.at[n], partner)

    per_half = half // COLS
    for n in range(out_pieces):
        pair_own(n).wait_recv()
        cross(n).wait_recv()
        h, columns = n // per_half, pl.ds((n % per_half) * COLS, COLS)
        total = (p_own[n, my_rows] + own_in[n]) + cross_in[n]
        out_ref[:, pl.ds(n * COLS, COLS)] = (x_mid[h, my_rows, columns].astype(jnp.float32) + total).astype(jnp.bfloat16)
        if next_q:
            next_x(n).start()

    if next_q:
        gain = q_gain_ref[pl.ds(layer + 1, 1), :]
        g_all[pl.ds(0, rows), :] = rms_scaled(out_ref[...], gain)
        for n in range(out_pieces):
            next_x(n).wait_recv()
        g_all[pl.ds(rows, rows), :] = rms_scaled(x_in[...], gain)
        for p in range(q_pairs):
            places, copies = wq_parts(p)
            for c in copies:
                c.wait()
            project_pair(
                p, g_all.at[pl.ds(0, chip_rows)], places, core, q_pairs, q_width // 2, partner, q_ref, q_send, q_ssem, q_rsem
            )

    for c in o_out:
        c.wait_send()
    x_out.wait_send()
    for j in range(x_pieces):
        to_partner(j).wait_send()
        to_across(j).wait_send()
        forward(j).wait_send()
    for n in range(out_pieces):
        pair_other(n).wait_send()
        cross(n).wait_send()
        pair_own(n).wait_send()
    if next_q:
        for n in range(out_pieces):
            next_x(n).wait_send()
        for p in range(q_pairs):
            give_pair(p, core, q_pairs, partner, q_ref, q_send, q_ssem, q_rsem).wait()


def tail(layer, o, x, gain, wo, wg_t, wu_t, wd, next_q):
    rows, d_model = x.shape
    hidden = wd.shape[1]
    width = o.shape[1]
    half = d_model // 2
    x_pieces, out_pieces, down_steps = half // COLS, d_model // COLS, d_model // DOWN
    steps = len(hidden_steps(hidden))
    dma = pltpu.SemaphoreType.DMA
    hbm = pl.BlockSpec(memory_space=pltpu.HBM)
    vmem = pl.BlockSpec(memory_space=pltpu.VMEM)
    in_specs = [vmem, hbm, hbm, hbm, hbm, hbm, hbm]
    out_shape = [jax.ShapeDtypeStruct((rows, d_model), jnp.bfloat16)]
    piece = pltpu.VMEM((out_pieces, rows, COLS), jnp.float32)
    scratch = [
        pltpu.VMEM((2 * rows, width), jnp.bfloat16),
        pltpu.VMEM((2 * rows, half), jnp.bfloat16),
        pltpu.VMEM((2, hidden, d_model), jnp.bfloat16),
        pltpu.VMEM((down_steps, hidden, DOWN), jnp.bfloat16),
        pltpu.VMEM((2, 4 * rows, half), jnp.bfloat16),
        pltpu.VMEM((4 * rows, d_model), jnp.bfloat16),
        pltpu.VMEM((4 * rows, hidden), jnp.bfloat16),
        pltpu.VMEM((out_pieces, 2 * rows, COLS), jnp.float32),
        pltpu.VMEM((out_pieces, 2 * rows, COLS), jnp.float32),
        piece, piece, piece, pltpu.VMEM(gain.shape, jnp.float32),
        dma((O_PARTS + 3,)), dma((x_pieces, O_PARTS)), dma((2, steps)), dma((down_steps,)),
        dma((O_PARTS,)), dma((O_PARTS,)), dma, dma,
        dma((x_pieces,)), dma((x_pieces,)), dma((x_pieces,)), dma((x_pieces,)), dma((x_pieces,)), dma((x_pieces,)),
        dma((out_pieces,)), dma((out_pieces,)), dma((out_pieces,)), dma((out_pieces,)), dma((out_pieces,)), dma((out_pieces,)),
    ]
    operands = [o, x, gain, wo, wg_t, wu_t, wd]
    if next_q is not None:
        q_gain, wq, heads = next_q
        kv_dim, pairs = wq.shape[2] // heads, heads // 4
        operands += [q_gain, wq]
        in_specs += [hbm, hbm]
        out_shape.append(jax.ShapeDtypeStruct((-(-kv_dim // LANES), heads * rows, LANES), jnp.float32))
        scratch += [
            pltpu.VMEM((d_model, 2 * (4 * kv_dim - d_model)), jnp.bfloat16),
            pltpu.VMEM((pairs, -(-kv_dim // LANES), 2 * rows, LANES), jnp.float32),
            pltpu.VMEM((rows, d_model), jnp.bfloat16),
            pltpu.VMEM(q_gain.shape, jnp.float32),
            dma((pairs, 2)), dma((out_pieces,)), dma((out_pieces,)), dma((pairs,)), dma((pairs,)),
        ]
    return pl.pallas_call(
        functools.partial(tail_kernel, layer, next_q is not None),
        out_shape=out_shape,
        in_specs=in_specs,
        out_specs=[vmem] * len(out_shape),
        scratch_shapes=scratch,
        compiler_params=pltpu.CompilerParams(collective_id=layer, has_side_effects=True, vmem_limit_bytes=49 * MIB),
        name=f'tail_{layer}',
    )(*operands)


def solution(mesh):
    row_axes = ('replica', 'dp')

    def local_step(x_rows, len_rows, cache, attn_gain, ffn_gain, w_query, w_attn_out, w_up, w_gate, w_down):
        layers, rows, _, kv_dim = cache.shape
        heads = w_query.shape[2] // kv_dim
        latent = w_attn_out.shape[1] // heads
        cache_t = jnp.swapaxes(cache, 2, 3)
        up_t, gate_t = jnp.swapaxes(w_up, 1, 2), jnp.swapaxes(w_gate, 1, 2)
        q = head(pltpu.with_memory_space_constraint(x_rows, pltpu.HBM), pltpu.with_memory_space_constraint(attn_gain, pltpu.HBM), w_query, heads)
        for layer in range(layers):
            mixed = attention(layer, q, len_rows, cache_t, rows, latent)
            next_q = (attn_gain, w_query, heads) if layer + 1 < layers else None
            outs = tail(layer, mixed, x_rows, ffn_gain, w_attn_out, gate_t, up_t, w_down, next_q)
            x_rows, q = outs[0], outs[-1]
        return x_rows

    return jax.shard_map(
        local_step,
        mesh=mesh,
        in_specs=(P(row_axes, None), P(row_axes), P(None, row_axes, None, None), P(), P(), P(), P(),
                  P(None, None, 'dp'), P(None, None, 'dp'), P(None, 'dp', None)),
        out_specs=P(row_axes, None),
        check_vma=False,
    )
```

```python
import functools

import jax
import jax.numpy as jnp
from jax import lax
from jax.experimental import pallas as pl
from jax.experimental.pallas import tpu as pltpu
from jax.sharding import PartitionSpec as P

NORM_EPS = 1e-6
MESH = pl.DeviceIdType.MESH
SEQS = 8
SLOTS = 3
TBLK = 128
PARTS = 2
COLS = 256
HID = 512
SUPER = 1280
DOWN = 512
O_PARTS = 4
MIB = 1024 * 1024
LANES = 128
BULK = 1


def remote_copy(src, dst, send, recv, device):
    return pltpu.make_async_remote_copy(
        src_ref=src, dst_ref=dst, send_sem=send, recv_sem=recv, device_id={'dp': device}, device_id_type=MESH
    )


def all_bytes(ref, sem):
    return pltpu.make_async_copy(ref, ref, sem)


def enter(*peers):
    barrier = pltpu.get_barrier_semaphore()
    for peer in peers:
        pl.semaphore_signal(barrier, inc=1, device_id={'dp': peer}, device_id_type=MESH)
    pl.semaphore_wait(barrier, len(peers))


def hidden_steps(hidden):
    ends = [min(start + SUPER, hidden) for start in range(0, hidden, SUPER)]
    return [(at, min(HID, end - at)) for t, end in enumerate(ends) for at in range(t * SUPER, end, HID)]


def rms_scaled(rows, gain):
    rows_f = rows.astype(jnp.float32)
    mean_sq = jnp.mean(rows_f * rows_f, axis=-1, keepdims=True)
    return (rows_f * lax.rsqrt(mean_sq + NORM_EPS) * gain).astype(jnp.bfloat16)


def project_pair(p, h_ref, parts, core, pairs, kv_dim, partner, q_ref, q_send, send_sem, recv_sem):
    rows = q_send.shape[2] // 2
    q = [jnp.dot(h_ref[...], part[...], preferred_element_type=jnp.float32) for part in parts]
    q = q[0] if len(q) == 1 else jnp.concatenate(q, axis=1)
    q = q.astype(jnp.bfloat16).astype(jnp.float32)
    for e in range(2):
        own = pl.ds(pl.multiple_of((core * pairs + p) * 2 * rows + e * rows, rows), rows)
        for c in range(q_ref.shape[0]):
            size = min(LANES, kv_dim - c * LANES)
            part = q[:, e * kv_dim + c * LANES :][:, :size]
            q_ref[c, own, pl.ds(0, size)] = part[:rows]
            q_send[p, c, pl.ds(e * rows, rows), pl.ds(0, size)] = part[rows:]
    give_pair(p, core, pairs, partner, q_ref, q_send, send_sem, recv_sem).start()


def give_pair(p, core, pairs, partner, q_ref, q_send, send_sem, recv_sem):
    size = q_send.shape[2]
    heads = pl.ds(pl.multiple_of((core * pairs + p) * size, size), size)
    return remote_copy(q_send.at[p], q_ref.at[:, heads], send_sem, recv_sem.at[p], partner)


def head_kernel(x_hbm, gain_hbm, wq_hbm, q_ref, x_ref, gain_ref, x_in, h_ref, wq, q_send, in_sem, wq_sem, x_send, x_recv, q_ssem, q_rsem):
    rows = x_hbm.shape[0]
    width = wq.shape[2]
    pairs = wq.shape[0]
    me = lax.axis_index('dp')
    core = lax.rem(me, 2)
    partner = me + 1 - 2 * core

    def wq_copy(p):
        columns = pl.ds(pl.multiple_of((core * pairs + p) * width, 128), width)
        return pltpu.make_async_copy(wq_hbm.at[0, :, columns], wq.at[p], wq_sem.at[p])

    x_own = pltpu.make_async_copy(x_hbm, x_ref, in_sem.at[0])
    gain_own = pltpu.make_async_copy(gain_hbm, gain_ref, in_sem.at[1])
    x_own.start()
    gain_own.start()
    for p in range(pairs):
        wq_copy(p).start(priority=BULK)
    x_own.wait()
    gain_own.wait()
    enter(partner)
    swap = remote_copy(x_ref, x_in, x_send, x_recv, partner)
    swap.start()
    h_ref[pl.ds(0, rows), :] = rms_scaled(x_ref[...], gain_ref[pl.ds(0, 1), :])
    swap.wait_recv()
    h_ref[pl.ds(rows, rows), :] = rms_scaled(x_in[...], gain_ref[pl.ds(0, 1), :])

    @pl.loop(0, pairs)
    def _(p):
        wq_copy(p).wait()
        project_pair(p, h_ref, [wq.at[p]], core, pairs, width // 2, partner, q_ref, q_send, q_ssem, q_rsem)

    swap.wait_send()
    for p in range(pairs):
        give_pair(p, core, pairs, partner, q_ref, q_send, q_ssem, q_rsem).wait_recv()
    all_bytes(q_send, q_ssem).wait()


def head(x, gain, wq, heads):
    rows, d_model = x.shape
    kv_dim = wq.shape[2] // heads
    pairs = heads // 4
    dma = pltpu.SemaphoreType.DMA
    vmem = pl.BlockSpec(memory_space=pltpu.VMEM)
    return pl.pallas_call(
        head_kernel,
        out_shape=jax.ShapeDtypeStruct((-(-kv_dim // LANES), heads * rows, LANES), jnp.float32),
        in_specs=[pl.BlockSpec(memory_space=pltpu.HBM)] * 3,
        out_specs=vmem,
        scratch_shapes=[
            pltpu.VMEM((rows, d_model), jnp.bfloat16),
            pltpu.VMEM(gain.shape, jnp.float32),
            pltpu.VMEM((rows, d_model), jnp.bfloat16),
            pltpu.VMEM((2 * rows, d_model), jnp.bfloat16),
            pltpu.VMEM((pairs, d_model, 2 * kv_dim), jnp.bfloat16),
            pltpu.VMEM((pairs, -(-kv_dim // LANES), 2 * rows, LANES), jnp.float32),
            dma((2,)), dma((pairs,)), dma, dma, dma, dma((pairs,)),
        ],
        compiler_params=pltpu.CompilerParams(collective_id=7, has_side_effects=True, vmem_limit_bytes=48 * MIB),
        name='head',
    )(x, gain, wq)


def attention_kernel(layer, scale, len_ref, q_ref, cache_ref, o_ref, buf, score_buf, prob_buf, o_buf, sem):
    rows = o_ref.shape[0]
    heads = q_ref.shape[1] // rows
    kv_dim, seq_len = cache_ref.shape[2:]
    latent = o_ref.shape[1] // heads
    groups = rows // SEQS
    max_blocks = seq_len // TBLK

    def blocks_of(group):
        longest = len_ref[group * SEQS]
        for i in range(1, SEQS):
            longest = jnp.maximum(longest, len_ref[group * SEQS + i])
        return lax.div(longest + (TBLK - 1), TBLK)

    def copy(group, slot, n):
        return pltpu.make_async_copy(
            cache_ref.at[layer, pl.ds(group * SEQS, SEQS), :, pl.ds(0, n * TBLK)],
            buf.at[slot, :, :, pl.ds(0, n * TBLK)],
            sem.at[slot],
        )

    def start(group, slot):
        blocks = blocks_of(group)
        for n in range(1, max_blocks + 1):

            @pl.when(blocks == n)
            def _():
                copy(group, slot, n).start()

    for group in range(min(SLOTS, groups)):
        start(group, group)

    def step(group, carry):
        slot = lax.rem(group, SLOTS)
        blocks = blocks_of(group)
        for n in range(1, max_blocks + 1):

            @pl.when(blocks == n)
            def _():
                copy(group, slot, n).wait()
                width = n * TBLK
                positions = lax.broadcasted_iota(jnp.int32, (heads, width), 1)
                for i in range(SEQS):
                    row = group * SEQS + i
                    query = [q_ref[c, pl.ds(row, heads, stride=rows), :] for c in range(q_ref.shape[0])]
                    query = jnp.concatenate(query, axis=1)[:, :kv_dim].astype(jnp.bfloat16)
                    score_buf[pl.ds(i * heads, heads), pl.ds(0, width)] = jnp.dot(
                        query, buf[slot, i, :, pl.ds(0, width)], preferred_element_type=jnp.float32
                    )
                for part in range(PARTS):
                    size = SEQS // PARTS
                    for i in range(part * size, (part + 1) * size):
                        row = group * SEQS + i
                        scores = score_buf[pl.ds(i * heads, heads), pl.ds(0, width)]
                        scores = jnp.where(positions < len_ref[row], scores * scale, -jnp.inf)
                        top = jnp.max(scores, axis=-1, keepdims=True)
                        probs = jnp.exp(scores - top)
                        probs = probs * (1.0 / jnp.sum(probs, axis=-1, keepdims=True))
                        prob_buf[pl.ds(i * heads, heads), pl.ds(0, width)] = probs.astype(jnp.bfloat16)
                    for i in range(part * size, (part + 1) * size):
                        row = group * SEQS + i
                        mixed = lax.dot_general(
                            prob_buf[pl.ds(i * heads, heads), pl.ds(0, width)],
                            buf[slot, i, pl.ds(0, latent), pl.ds(0, width)],
                            (((1,), (1,)), ((), ())),
                            preferred_element_type=jnp.float32,
                        )
                        for c in range(latent // LANES):
                            place = pl.ds(pl.multiple_of(row * heads, heads), heads)
                            o_buf[c, place, :] = mixed[:, c * LANES : (c + 1) * LANES]

        @pl.when(group + SLOTS < groups)
        def _():
            start(group + SLOTS, slot)

        return carry

    lax.fori_loop(0, groups, step, 0)
    for h in range(heads):
        for c in range(latent // LANES):
            place = pl.ds(h * latent + c * LANES, LANES)
            o_ref[:, place] = o_buf[c, pl.ds(h, rows, stride=heads), :].astype(jnp.bfloat16)


def attention(layer, q, lengths, cache_t, rows, latent):
    heads = q.shape[1] // rows
    kv_dim, seq_len = cache_t.shape[2:]
    scale = (3 * (kv_dim - latent)) ** -0.5
    return pl.pallas_call(
        functools.partial(attention_kernel, layer, scale),
        out_shape=jax.ShapeDtypeStruct((rows, heads * latent), jnp.bfloat16),
        in_specs=[
            pl.BlockSpec(memory_space=pltpu.SMEM),
            pl.BlockSpec(memory_space=pltpu.VMEM),
            pl.BlockSpec(memory_space=pl.ANY),
        ],
        out_specs=pl.BlockSpec(memory_space=pltpu.VMEM),
        scratch_shapes=[
            pltpu.VMEM((SLOTS, SEQS, kv_dim, seq_len), jnp.bfloat16),
            pltpu.VMEM((SEQS * heads, seq_len), jnp.float32),
            pltpu.VMEM((SEQS * heads, seq_len), jnp.bfloat16),
            pltpu.VMEM((latent // LANES, rows * heads, LANES), jnp.float32),
            pltpu.SemaphoreType.DMA((SLOTS,)),
        ],
        compiler_params=pltpu.CompilerParams(vmem_limit_bytes=40 * MIB),
        name=f'attention_{layer}',
    )(lengths, q, cache_t)


def tail_kernel(layer, next_q, *refs):
    refs = list(refs)

    def take(count):
        taken, refs[:count] = refs[:count], []
        return taken

    o_ref, x_hbm, gain_hbm, wo_ref, wg_hbm, wu_hbm, wd_hbm = take(7)
    if next_q:
        q_gain_hbm, wq_hbm = take(2)
    (out_ref,) = take(1)
    if next_q:
        (q_ref,) = take(1)
    o_all, x_old, wgu, wd, x_mid, g_all, a_all, p_other, p_own, part_in, cross_in, own_in, gain_ref = take(13)
    in_sem, wo_sem, w_sem, wd_sem = take(4)
    o_send, o_recv, xo_send, xo_recv, xp_send, xp_recv, xc_send, xc_recv, xf_send, xf_recv = take(10)
    p1_send, p1_recv, p2_send, p2_recv, p3_send, p3_recv = take(6)
    if next_q:
        wq, q_send, x_in, q_gain_ref, wq_sem, x_send, x_recv, q_ssem, q_rsem = take(9)

    rows, d_model = x_hbm.shape
    chip_rows = 2 * rows
    half = d_model // 2
    hidden = wd_hbm.shape[1]
    o_width = o_ref.shape[1]
    o_part = o_width // O_PARTS
    x_pieces = half // COLS
    out_pieces = d_model // COLS
    steps = hidden_steps(hidden)
    loop_steps = -(-SUPER // HID)
    loops = hidden // SUPER

    me = lax.axis_index('dp')
    core = lax.rem(me, 2)
    partner = me + 1 - 2 * core
    across = lax.rem(me + 2, 4)
    other_core = 1 - core
    my_rows = pl.ds(pl.multiple_of(core * rows, rows), rows)
    partner_rows = pl.ds(pl.multiple_of(other_core * rows, rows), rows)

    wg, wu = wgu.at[0], wgu.at[1]
    per_region = x_pieces // 2

    def wo_place(j, k):
        lane = pl.multiple_of(lax.rem(j, per_region) * (O_PARTS * COLS) + k * COLS, COLS)
        return wgu.at[lax.div(j, per_region), pl.ds(0, o_part), pl.ds(lane, COLS)]

    def wo_copy(j, k):
        columns = pl.ds(pl.multiple_of(core * half + j * COLS, COLS), COLS)
        return pltpu.make_async_copy(
            wo_ref.at[layer, pl.ds(k * o_part, o_part), columns], wo_place(j, k), wo_sem.at[j]
        )

    def gate_copy(i):
        window = pl.ds(*steps[i])
        return pltpu.make_async_copy(wg_hbm.at[layer, window], wg.at[window], w_sem.at[i])

    def up_copy(i):
        window = pl.ds(*steps[i])
        return pltpu.make_async_copy(wu_hbm.at[layer, window], wu.at[window], w_sem.at[i])

    def down_copy(n):
        columns = pl.ds(n * DOWN, DOWN)
        return pltpu.make_async_copy(wd_hbm.at[layer, :, columns], wd.at[n], wd_sem.at[n])

    o_parts = [pl.ds(k * o_part, o_part) for k in range(O_PARTS)]
    o_own = [pltpu.make_async_copy(o_ref.at[:, w], o_all.at[my_rows, w], in_sem.at[k]) for k, w in enumerate(o_parts)]
    x_own = pltpu.make_async_copy(
        x_hbm.at[:, pl.ds(pl.multiple_of(core * half, half), half)], x_old.at[my_rows], in_sem.at[O_PARTS]
    )
    gains = [pltpu.make_async_copy(gain_hbm, gain_ref, in_sem.at[O_PARTS + 1])]
    if next_q:
        gains.append(pltpu.make_async_copy(q_gain_hbm, q_gain_ref, in_sem.at[O_PARTS + 2]))
    for c in o_own + [x_own] + gains:
        c.start()
    for j in range(x_pieces):
        for k in range(O_PARTS):
            wo_copy(j, k).start(priority=BULK)

    enter(partner, across)

    o_out = [remote_copy(o_ref.at[:, w], o_all.at[my_rows, w], o_send, o_recv.at[k], partner) for k, w in enumerate(o_parts)]
    x_out = remote_copy(
        x_hbm.at[:, pl.ds(pl.multiple_of(other_core * half, half), half)], x_old.at[my_rows], xo_send, xo_recv, partner
    )
    for c in o_out:
        c.start()
    x_out.start()

    def piece_of(j):
        return pl.ds(pl.multiple_of(j * COLS, COLS), COLS)

    def to_partner(j):
        piece = x_mid.at[core, pl.ds(0, chip_rows), piece_of(j)]
        return remote_copy(piece, piece, xp_send, xp_recv.at[j], partner)

    def to_across(j):
        src = x_mid.at[core, pl.ds(0, chip_rows), piece_of(j)]
        dst = x_mid.at[core, pl.ds(chip_rows, chip_rows), piece_of(j)]
        return remote_copy(src, dst, xc_send, xc_recv.at[j], across)

    def forward(j):
        piece = x_mid.at[core, pl.ds(chip_rows, chip_rows), pl.ds(j * COLS, COLS)]
        return remote_copy(piece, piece, xf_send, xf_recv.at[j], partner)

    def o_dot(j, k):
        return jnp.dot(o_all[:, o_parts[k]], wo_place(j, k)[...], preferred_element_type=jnp.float32)

    def finish_piece(j, product):
        columns = piece_of(j)
        x_mid[core, pl.ds(0, chip_rows), columns] = (x_old[:, columns].astype(jnp.float32) + product).astype(jnp.bfloat16)
        to_across(j).start()
        to_partner(j).start()

    for c in [x_own] + gains + o_own:
        c.wait()
    for c in [x_out] + o_out:
        c.wait_recv()

    @pl.loop(0, x_pieces)
    def _(j):
        all_bytes(wgu.at[0, pl.ds(0, o_part), pl.ds(0, O_PARTS * COLS)], wo_sem.at[j]).wait()
        finish_piece(j, functools.reduce(jnp.add, [o_dot(j, k) for k in range(O_PARTS)]))

        @pl.when(j == 0)
        def _():
            down_copy(0).start(priority=BULK)

        @pl.when(j == per_region)
        def _():
            down_copy(1).start(priority=BULK)

        for at in range(2):

            @pl.when(j == (at + 1) * per_region - 1)
            def _():
                for i in range(len(steps)):
                    (gate_copy, up_copy)[at](i).start(priority=BULK)

    for n in range(2, d_model // DOWN):
        down_copy(n).start(priority=BULK)

    if next_q:
        q_pairs = q_rsem.shape[0]
        q_width = wq_hbm.shape[2] // (2 * q_pairs)
        spare = d_model - q_width
        over = q_width - spare

        def wq_parts(p):
            region = (wg, wu)[p % 2]
            spans = [(region, 0, 0, q_width)] if p < 2 else [(region, q_width, 0, spare), (wq, (p % 2) * over, spare, over)]
            return [(buffer.at[pl.ds(0, d_model), pl.ds(lane, size)], offset, size) for buffer, lane, offset, size in spans]

        def wq_start(p):
            for place, offset, size in wq_parts(p):
                columns = pl.ds(pl.multiple_of((core * q_pairs + p) * q_width + offset, LANES), size)
                pltpu.make_async_copy(wq_hbm.at[layer + 1, :, columns], place, wq_sem.at[p]).start(priority=BULK)

    def normalize(start):
        window = pl.ds(start, chip_rows)
        halves = [x_mid[h, window, :].astype(jnp.float32) for h in range(2)]
        total = sum(jnp.sum(v * v, axis=-1, keepdims=True) for v in halves)
        factor = lax.rsqrt(total * (1.0 / d_model) + NORM_EPS)
        for h in range(2):
            gain = gain_ref[pl.ds(layer, 1), pl.ds(h * half, half)]
            g_all[window, pl.ds(h * half, half)] = (halves[h] * factor * gain).astype(jnp.bfloat16)

    for j in range(x_pieces):
        to_partner(j).wait_recv()
    normalize(0)
    for j in range(x_pieces):
        to_across(j).wait_recv()
        forward(j).start()
    for j in range(x_pieces):
        forward(j).wait_recv()
    normalize(chip_rows)

    def gate_up(i, start, size):
        window = pl.ds(start, size)
        all_bytes(wgu.at[:, window], w_sem.at[i]).wait()
        dims = (((1,), (1,)), ((), ()))
        gate = lax.dot_general(g_all[...], wg[window, :], dims, preferred_element_type=jnp.float32)
        up = lax.dot_general(g_all[...], wu[window, :], dims, preferred_element_type=jnp.float32)
        a_all[:, window] = (jax.nn.silu(gate) * up).astype(jnp.bfloat16)

    @pl.loop(0, loops)
    def _(t):
        for i in range(loop_steps):
            start, size = steps[i]
            gate_up(t * loop_steps + i, pl.multiple_of(t * SUPER + start, LANES), size)

    for i in range(loops * loop_steps, len(steps)):
        gate_up(i, *steps[i])

    if next_q:
        for p in range(q_pairs):
            wq_start(p)

    def pair_other(n):
        return remote_copy(p_other.at[n, partner_rows], part_in.at[n], p1_send, p1_recv.at[n], partner)

    def cross(n):
        return remote_copy(part_in.at[n], cross_in.at[n], p2_send, p2_recv.at[n], across)

    def pair_own(n):
        return remote_copy(p_own.at[n, partner_rows], own_in.at[n], p3_send, p3_recv.at[n], partner)

    def send_sum(n):
        pair_other(n).wait_recv()
        part_in[n] = p_other[n, my_rows] + part_in[n]
        cross(n).start()

    per_step = DOWN // COLS
    down_steps = d_model // DOWN
    for d in range(down_steps):
        down_copy(d).wait()
    spans = [(0, COLS), (COLS, COLS)] + [(at, DOWN) for at in range(DOWN, d_model, DOWN)]
    given, summed = 0, 0
    for t, (at, size) in enumerate(spans):
        weight = wd[at // DOWN, :, pl.ds(at % DOWN, size)]
        product = jnp.dot(a_all[pl.ds(chip_rows, chip_rows), :], weight, preferred_element_type=jnp.float32)
        ready = 0 if t < 2 else 1 if t == 2 else given
        for e in range(size // COLS):
            p_other[given] = product[:, e * COLS : (e + 1) * COLS]
            pair_other(given).start()
            given += 1
        for n in range(summed, ready):
            send_sum(n)
        summed = max(summed, ready)
    @pl.loop(0, down_steps)
    def _(d):
        @pl.when(d == 0)
        def _():
            for n in range(summed, out_pieces):
                send_sum(n)

        product = jnp.dot(a_all[pl.ds(0, chip_rows), :], wd[d], preferred_element_type=jnp.float32)
        for e in range(per_step):
            n = d * per_step + e
            p_own[n] = product[:, e * COLS : (e + 1) * COLS]
            pair_own(n).start()

    def next_x(n):
        piece = pl.ds(n * COLS, COLS)
        return remote_copy(out_ref.at[:, piece], x_in.at[:, piece], x_send, x_recv.at[n], partner)

    per_half = half // COLS
    for n in range(out_pieces):
        pair_own(n).wait_recv()
        cross(n).wait_recv()
        h, columns = n // per_half, pl.ds((n % per_half) * COLS, COLS)
        total = (p_own[n, my_rows] + own_in[n]) + cross_in[n]
        out_ref[:, pl.ds(n * COLS, COLS)] = (x_mid[h, my_rows, columns].astype(jnp.float32) + total).astype(jnp.bfloat16)
        if next_q:
            next_x(n).start()

    if next_q:
        gain = q_gain_ref[pl.ds(layer + 1, 1), :]
        g_all[pl.ds(0, rows), :] = rms_scaled(out_ref[...], gain)
        for n in range(out_pieces):
            next_x(n).wait_recv()
        g_all[pl.ds(rows, rows), :] = rms_scaled(x_in[...], gain)
        for p in range(q_pairs):
            places = [place for place, _, _ in wq_parts(p)]
            all_bytes(wg.at[pl.ds(0, d_model), pl.ds(0, q_width)], wq_sem.at[p]).wait()
            project_pair(
                p, g_all.at[pl.ds(0, chip_rows)], places, core, q_pairs, q_width // 2, partner, q_ref, q_send, q_ssem, q_rsem
            )

    x_out.wait_send()
    all_bytes(o_ref, o_send).wait()
    for sem in (xp_send, xc_send, xf_send):
        all_bytes(x_mid.at[0, pl.ds(0, chip_rows)], sem).wait()
    for sem in (p1_send, p2_send, p3_send):
        all_bytes(cross_in, sem).wait()
    if next_q:
        all_bytes(out_ref, x_send).wait()
        for p in range(q_pairs):
            give_pair(p, core, q_pairs, partner, q_ref, q_send, q_ssem, q_rsem).wait_recv()
        all_bytes(q_send, q_ssem).wait()


def tail(layer, o, x, gain, wo, wg_t, wu_t, wd, next_q):
    rows, d_model = x.shape
    hidden = wd.shape[1]
    width = o.shape[1]
    half = d_model // 2
    x_pieces, out_pieces, down_steps = half // COLS, d_model // COLS, d_model // DOWN
    steps = len(hidden_steps(hidden))
    dma = pltpu.SemaphoreType.DMA
    hbm = pl.BlockSpec(memory_space=pltpu.HBM)
    vmem = pl.BlockSpec(memory_space=pltpu.VMEM)
    in_specs = [vmem, hbm, hbm, hbm, hbm, hbm, hbm]
    out_shape = [jax.ShapeDtypeStruct((rows, d_model), jnp.bfloat16)]
    piece = pltpu.VMEM((out_pieces, rows, COLS), jnp.float32)
    scratch = [
        pltpu.VMEM((2 * rows, width), jnp.bfloat16),
        pltpu.VMEM((2 * rows, half), jnp.bfloat16),
        pltpu.VMEM((2, hidden, d_model), jnp.bfloat16),
        pltpu.VMEM((down_steps, hidden, DOWN), jnp.bfloat16),
        pltpu.VMEM((2, 4 * rows, half), jnp.bfloat16),
        pltpu.VMEM((4 * rows, d_model), jnp.bfloat16),
        pltpu.VMEM((4 * rows, hidden), jnp.bfloat16),
        pltpu.VMEM((out_pieces, 2 * rows, COLS), jnp.float32),
        pltpu.VMEM((out_pieces, 2 * rows, COLS), jnp.float32),
        piece, piece, piece, pltpu.VMEM(gain.shape, jnp.float32),
        dma((O_PARTS + 3,)), dma((x_pieces,)), dma((steps,)), dma((down_steps,)),
        dma, dma((O_PARTS,)), dma, dma,
        dma, dma((x_pieces,)), dma, dma((x_pieces,)), dma, dma((x_pieces,)),
        dma, dma((out_pieces,)), dma, dma((out_pieces,)), dma, dma((out_pieces,)),
    ]
    operands = [o, x, gain, wo, wg_t, wu_t, wd]
    if next_q is not None:
        q_gain, wq, heads = next_q
        kv_dim, pairs = wq.shape[2] // heads, heads // 4
        operands += [q_gain, wq]
        in_specs += [hbm, hbm]
        out_shape.append(jax.ShapeDtypeStruct((-(-kv_dim // LANES), heads * rows, LANES), jnp.float32))
        scratch += [
            pltpu.VMEM((d_model, 2 * (4 * kv_dim - d_model)), jnp.bfloat16),
            pltpu.VMEM((pairs, -(-kv_dim // LANES), 2 * rows, LANES), jnp.float32),
            pltpu.VMEM((rows, d_model), jnp.bfloat16),
            pltpu.VMEM(q_gain.shape, jnp.float32),
            dma((pairs,)), dma, dma((out_pieces,)), dma, dma((pairs,)),
        ]
    return pl.pallas_call(
        functools.partial(tail_kernel, layer, next_q is not None),
        out_shape=out_shape,
        in_specs=in_specs,
        out_specs=[vmem] * len(out_shape),
        scratch_shapes=scratch,
        compiler_params=pltpu.CompilerParams(collective_id=layer, has_side_effects=True, vmem_limit_bytes=49 * MIB),
        name=f'tail_{layer}',
    )(*operands)


def solution(mesh):
    row_axes = ('replica', 'dp')

    def local_step(x_rows, len_rows, cache, attn_gain, ffn_gain, w_query, w_attn_out, w_up, w_gate, w_down):
        layers, rows, _, kv_dim = cache.shape
        heads = w_query.shape[2] // kv_dim
        latent = w_attn_out.shape[1] // heads
        cache_t = jnp.swapaxes(cache, 2, 3)
        up_t, gate_t = jnp.swapaxes(w_up, 1, 2), jnp.swapaxes(w_gate, 1, 2)
        q = head(pltpu.with_memory_space_constraint(x_rows, pltpu.HBM), pltpu.with_memory_space_constraint(attn_gain, pltpu.HBM), w_query, heads)
        for layer in range(layers):
            mixed = attention(layer, q, len_rows, cache_t, rows, latent)
            next_q = (attn_gain, w_query, heads) if layer + 1 < layers else None
            outs = tail(layer, mixed, x_rows, ffn_gain, w_attn_out, gate_t, up_t, w_down, next_q)
            x_rows, q = outs[0], outs[-1]
        return x_rows

    return jax.shard_map(
        local_step,
        mesh=mesh,
        in_specs=(P(row_axes, None), P(row_axes), P(None, row_axes, None, None), P(), P(), P(), P(),
                  P(None, None, 'dp'), P(None, None, 'dp'), P(None, 'dp', None)),
        out_specs=P(row_axes, None),
        check_vma=False,
    )
```

```python
import functools

import jax
import jax.numpy as jnp
from jax import lax
from jax.experimental import pallas as pl
from jax.experimental.pallas import tpu as pltpu
from jax.sharding import PartitionSpec as P

NORM_EPS = 1e-6
MESH = pl.DeviceIdType.MESH
SEQS = 8
SLOTS = 3
TBLK = 128
PARTS = 2
COLS = 256
HID = 512
SUPER = 1280
DOWN = 512
O_PARTS = 4
MIB = 1024 * 1024
LANES = 128
BULK = 1


def remote_copy(src, dst, send, recv, device):
    return pltpu.make_async_remote_copy(
        src_ref=src, dst_ref=dst, send_sem=send, recv_sem=recv, device_id={'dp': device}, device_id_type=MESH
    )


def all_bytes(ref, sem):
    return pltpu.make_async_copy(ref, ref, sem)


def enter(*peers):
    barrier = pltpu.get_barrier_semaphore()
    for peer in peers:
        pl.semaphore_signal(barrier, inc=1, device_id={'dp': peer}, device_id_type=MESH)
    pl.semaphore_wait(barrier, len(peers))


def hidden_steps(hidden):
    ends = [min(start + SUPER, hidden) for start in range(0, hidden, SUPER)]
    return [(at, min(HID, end - at)) for t, end in enumerate(ends) for at in range(t * SUPER, end, HID)]


def rms_scaled(rows, gain):
    rows_f = rows.astype(jnp.float32)
    mean_sq = jnp.mean(rows_f * rows_f, axis=-1, keepdims=True)
    return (rows_f * lax.rsqrt(mean_sq + NORM_EPS) * gain).astype(jnp.bfloat16)


def project_pair(p, h_ref, parts, core, pairs, kv_dim, partner, q_ref, q_send, q_in, send_sem, recv_sem):
    rows = q_send.shape[2] // 2
    q = [jnp.dot(h_ref[...], part[...], preferred_element_type=jnp.float32) for part in parts]
    q = q[0] if len(q) == 1 else jnp.concatenate(q, axis=1)
    q = q.astype(jnp.bfloat16)
    for e in range(2):
        own = pl.ds(pl.multiple_of((core * pairs + p) * 2 * rows + e * rows, rows), rows)
        for c in range(q_ref.shape[0]):
            size = min(LANES, kv_dim - c * LANES)
            part = q[:, e * kv_dim + c * LANES :][:, :size]
            q_ref[c, own, pl.ds(0, size)] = part[:rows].astype(jnp.float32)
            q_send[p, c, pl.ds(e * rows, rows), pl.ds(0, size)] = part[rows:]
    remote_copy(q_send.at[p], q_in.at[p], send_sem, recv_sem.at[p], partner).start()


def receive_pairs(core, pairs, partner, q_ref, q_send, q_in, send_sem, recv_sem):
    size = q_send.shape[2]
    for p in range(pairs):
        remote_copy(q_send.at[p], q_in.at[p], send_sem, recv_sem.at[p], partner).wait_recv()
        theirs = pl.ds(pl.multiple_of(((1 - core) * pairs + p) * size, size), size)
        q_ref[:, theirs, :] = q_in[p].astype(jnp.float32)
    all_bytes(q_send, send_sem).wait()


def head_kernel(x_hbm, gain_hbm, wq_hbm, q_ref, x_ref, gain_ref, x_in, h_ref, wq, q_send, q_in, in_sem, wq_sem, x_send, x_recv, q_ssem, q_rsem):
    rows = x_hbm.shape[0]
    width = wq.shape[2]
    pairs = wq.shape[0]
    me = lax.axis_index('dp')
    core = lax.rem(me, 2)
    partner = me + 1 - 2 * core

    def wq_copy(p):
        columns = pl.ds(pl.multiple_of((core * pairs + p) * width, 128), width)
        return pltpu.make_async_copy(wq_hbm.at[0, :, columns], wq.at[p], wq_sem.at[p])

    x_own = pltpu.make_async_copy(x_hbm, x_ref, in_sem.at[0])
    gain_own = pltpu.make_async_copy(gain_hbm, gain_ref, in_sem.at[1])
    x_own.start()
    gain_own.start()
    for p in range(pairs):
        wq_copy(p).start(priority=BULK)
    x_own.wait()
    gain_own.wait()
    enter(partner)
    swap = remote_copy(x_ref, x_in, x_send, x_recv, partner)
    swap.start()
    h_ref[pl.ds(0, rows), :] = rms_scaled(x_ref[...], gain_ref[pl.ds(0, 1), :])
    swap.wait_recv()
    h_ref[pl.ds(rows, rows), :] = rms_scaled(x_in[...], gain_ref[pl.ds(0, 1), :])

    @pl.loop(0, pairs)
    def _(p):
        wq_copy(p).wait()
        project_pair(p, h_ref, [wq.at[p]], core, pairs, width // 2, partner, q_ref, q_send, q_in, q_ssem, q_rsem)

    swap.wait_send()
    receive_pairs(core, pairs, partner, q_ref, q_send, q_in, q_ssem, q_rsem)


def head(x, gain, wq, heads):
    rows, d_model = x.shape
    kv_dim = wq.shape[2] // heads
    pairs = heads // 4
    dma = pltpu.SemaphoreType.DMA
    vmem = pl.BlockSpec(memory_space=pltpu.VMEM)
    return pl.pallas_call(
        head_kernel,
        out_shape=jax.ShapeDtypeStruct((-(-kv_dim // LANES), heads * rows, LANES), jnp.float32),
        in_specs=[pl.BlockSpec(memory_space=pltpu.HBM)] * 3,
        out_specs=vmem,
        scratch_shapes=[
            pltpu.VMEM((rows, d_model), jnp.bfloat16),
            pltpu.VMEM(gain.shape, jnp.float32),
            pltpu.VMEM((rows, d_model), jnp.bfloat16),
            pltpu.VMEM((2 * rows, d_model), jnp.bfloat16),
            pltpu.VMEM((pairs, d_model, 2 * kv_dim), jnp.bfloat16),
            pltpu.VMEM((pairs, -(-kv_dim // LANES), 2 * rows, LANES), jnp.bfloat16),
            pltpu.VMEM((pairs, -(-kv_dim // LANES), 2 * rows, LANES), jnp.bfloat16),
            dma((2,)), dma((pairs,)), dma, dma, dma, dma((pairs,)),
        ],
        compiler_params=pltpu.CompilerParams(collective_id=7, has_side_effects=True, vmem_limit_bytes=48 * MIB),
        name='head',
    )(x, gain, wq)


def attention_kernel(layer, scale, len_ref, q_ref, cache_ref, o_ref, buf, score_buf, prob_buf, o_buf, q_buf, sem):
    rows = o_ref.shape[0]
    heads = q_ref.shape[1] // rows
    kv_dim, seq_len = cache_ref.shape[2:]
    latent = o_ref.shape[1] // heads
    groups = rows // SEQS
    max_blocks = seq_len // TBLK
    split = latent // 2
    dims = (((1,), (1,)), ((), ()))

    def blocks_of(group):
        longest = len_ref[group * SEQS]
        for i in range(1, SEQS):
            longest = jnp.maximum(longest, len_ref[group * SEQS + i])
        return lax.div(longest + (TBLK - 1), TBLK)

    def copy(group, slot, n):
        return pltpu.make_async_copy(
            cache_ref.at[layer, pl.ds(group * SEQS, SEQS), :, pl.ds(0, n * TBLK)],
            buf.at[slot, :, :, pl.ds(0, n * TBLK)],
            sem.at[slot],
        )

    def start(group, slot):
        blocks = blocks_of(group)
        for n in range(1, max_blocks + 1):

            @pl.when(blocks == n)
            def _():
                copy(group, slot, n).start()

    for group in range(min(SLOTS, groups)):
        start(group, group)

    def pack(group):
        out_rows = pl.ds(pl.multiple_of(group * SEQS, SEQS), SEQS)
        for h in range(heads):
            for c in range(latent // LANES):
                source = pl.ds(group * (SEQS * heads) + h, SEQS, stride=heads)
                o_ref[out_rows, pl.ds(h * latent + c * LANES, LANES)] = o_buf[c, source, :].astype(jnp.bfloat16)

    def step(group, carry):
        slot = lax.rem(group, SLOTS)
        blocks = blocks_of(group)
        for n in range(1, max_blocks + 1):

            @pl.when(blocks == n)
            def _():
                copy(group, slot, n).wait()
                width = n * TBLK
                pack(jnp.maximum(group - 1, 0))
                positions = lax.broadcasted_iota(jnp.int32, (heads, width), 1)
                for i in range(SEQS):
                    row = group * SEQS + i
                    query = q_buf[row]
                    score_buf[pl.ds(i * heads, heads), pl.ds(0, width)] = jnp.dot(
                        query, buf[slot, i, :, pl.ds(0, width)], preferred_element_type=jnp.float32
                    )
                for part in range(PARTS):
                    size = SEQS // PARTS
                    for i in range(part * size, (part + 1) * size):
                        row = group * SEQS + i
                        scores = score_buf[pl.ds(i * heads, heads), pl.ds(0, width)]
                        scores = jnp.where(positions < len_ref[row], scores * scale, -jnp.inf)
                        top = jnp.max(scores, axis=-1, keepdims=True)
                        probs = jnp.exp(scores - top)
                        probs = probs * (1.0 / jnp.sum(probs, axis=-1, keepdims=True))
                        prob_buf[pl.ds(i * heads, heads), pl.ds(0, width)] = probs.astype(jnp.bfloat16)
                    for i in range(part * size, (part + 1) * size):
                        row = group * SEQS + i
                        probs = prob_buf[pl.ds(i * heads, heads), pl.ds(0, width)]
                        low = buf[slot, i, pl.ds(0, split), pl.ds(0, width)]
                        high = buf[slot, i, pl.ds(split, latent - split), pl.ds(0, width)]
                        low = lax.dot_general(probs, low, dims, preferred_element_type=jnp.float32)
                        high = lax.dot_general(high, probs, dims, preferred_element_type=jnp.float32)
                        mixed = jnp.concatenate([low, high.T], axis=1)
                        for c in range(latent // LANES):
                            place = pl.ds(pl.multiple_of(row * heads, heads), heads)
                            o_buf[c, place, :] = mixed[:, c * LANES : (c + 1) * LANES]

        @pl.when(group + SLOTS < groups)
        def _():
            start(group + SLOTS, slot)

        return carry

    @pl.loop(0, groups)
    def _(group):
        for i in range(SEQS):
            row = group * SEQS + i
            query = [q_ref[c, pl.ds(row, heads, stride=rows), :] for c in range(q_ref.shape[0])]
            q_buf[row] = jnp.concatenate(query, axis=1)[:, :kv_dim].astype(jnp.bfloat16)

    lax.fori_loop(0, groups, step, 0)
    pack(groups - 1)


def attention(layer, q, lengths, cache_t, rows, latent):
    heads = q.shape[1] // rows
    kv_dim, seq_len = cache_t.shape[2:]
    scale = (3 * (kv_dim - latent)) ** -0.5
    return pl.pallas_call(
        functools.partial(attention_kernel, layer, scale),
        out_shape=jax.ShapeDtypeStruct((rows, heads * latent), jnp.bfloat16),
        in_specs=[
            pl.BlockSpec(memory_space=pltpu.SMEM),
            pl.BlockSpec(memory_space=pltpu.VMEM),
            pl.BlockSpec(memory_space=pl.ANY),
        ],
        out_specs=pl.BlockSpec(memory_space=pltpu.VMEM),
        scratch_shapes=[
            pltpu.VMEM((SLOTS, SEQS, kv_dim, seq_len), jnp.bfloat16),
            pltpu.VMEM((SEQS * heads, seq_len), jnp.float32),
            pltpu.VMEM((SEQS * heads, seq_len), jnp.bfloat16),
            pltpu.VMEM((latent // LANES, rows * heads, LANES), jnp.float32),
            pltpu.VMEM((rows, heads, kv_dim), jnp.bfloat16),
            pltpu.SemaphoreType.DMA((SLOTS,)),
        ],
        compiler_params=pltpu.CompilerParams(vmem_limit_bytes=40 * MIB),
        name=f'attention_{layer}',
    )(lengths, q, cache_t)


def tail_kernel(layer, next_q, *refs):
    refs = list(refs)

    def take(count):
        taken, refs[:count] = refs[:count], []
        return taken

    o_ref, x_hbm, gain_hbm, wo_ref, wg_hbm, wu_hbm, wd_hbm = take(7)
    if next_q:
        q_gain_hbm, wq_hbm = take(2)
    (out_ref,) = take(1)
    if next_q:
        (q_ref,) = take(1)
    o_all, x_old, wgu, wd, x_mid, g_all, a_all, p_other, p_own, part_in, cross_in, own_in, gain_ref = take(13)
    in_sem, wo_sem, w_sem, wd_sem = take(4)
    o_send, o_recv, xo_send, xo_recv, xp_send, xp_recv, xc_send, xc_recv, xf_send, xf_recv = take(10)
    p1_send, p1_recv, p2_send, p2_recv, p3_send, p3_recv = take(6)
    if next_q:
        wq, q_send, q_in, x_in, q_gain_ref, wq_sem, x_send, x_recv, q_ssem, q_rsem = take(10)

    rows, d_model = x_hbm.shape
    chip_rows = 2 * rows
    half = d_model // 2
    hidden = wd_hbm.shape[1]
    o_width = o_ref.shape[1]
    o_part = o_width // O_PARTS
    x_pieces = half // COLS
    out_pieces = d_model // COLS
    steps = hidden_steps(hidden)
    loop_steps = -(-SUPER // HID)
    loops = hidden // SUPER

    me = lax.axis_index('dp')
    core = lax.rem(me, 2)
    partner = me + 1 - 2 * core
    across = lax.rem(me + 2, 4)
    other_core = 1 - core
    my_rows = pl.ds(pl.multiple_of(core * rows, rows), rows)
    partner_rows = pl.ds(pl.multiple_of(other_core * rows, rows), rows)

    wg, wu = wgu.at[0], wgu.at[1]
    per_region = x_pieces // 2

    def wo_place(j, k):
        lane = pl.multiple_of(lax.rem(j, per_region) * (O_PARTS * COLS) + k * COLS, COLS)
        return wgu.at[lax.div(j, per_region), pl.ds(0, o_part), pl.ds(lane, COLS)]

    def wo_copy(j, k):
        columns = pl.ds(pl.multiple_of(core * half + j * COLS, COLS), COLS)
        return pltpu.make_async_copy(
            wo_ref.at[layer, pl.ds(k * o_part, o_part), columns], wo_place(j, k), wo_sem.at[j]
        )

    def gate_copy(i):
        window = pl.ds(*steps[i])
        return pltpu.make_async_copy(wg_hbm.at[layer, window], wg.at[window], w_sem.at[i])

    def up_copy(i):
        window = pl.ds(*steps[i])
        return pltpu.make_async_copy(wu_hbm.at[layer, window], wu.at[window], w_sem.at[i])

    def down_copy(n):
        columns = pl.ds(n * DOWN, DOWN)
        return pltpu.make_async_copy(wd_hbm.at[layer, :, columns], wd.at[n], wd_sem.at[n])

    o_parts = [pl.ds(k * o_part, o_part) for k in range(O_PARTS)]
    o_own = [pltpu.make_async_copy(o_ref.at[:, w], o_all.at[my_rows, w], in_sem.at[k]) for k, w in enumerate(o_parts)]
    x_own = pltpu.make_async_copy(
        x_hbm.at[:, pl.ds(pl.multiple_of(core * half, half), half)], x_old.at[my_rows], in_sem.at[O_PARTS]
    )
    gains = [pltpu.make_async_copy(gain_hbm, gain_ref, in_sem.at[O_PARTS + 1])]
    if next_q:
        gains.append(pltpu.make_async_copy(q_gain_hbm, q_gain_ref, in_sem.at[O_PARTS + 2]))
    for c in o_own + [x_own] + gains:
        c.start()
    for j in range(x_pieces):
        for k in range(O_PARTS):
            wo_copy(j, k).start(priority=BULK)

    enter(partner, across)

    o_out = [remote_copy(o_ref.at[:, w], o_all.at[my_rows, w], o_send, o_recv.at[k], partner) for k, w in enumerate(o_parts)]
    x_out = remote_copy(
        x_hbm.at[:, pl.ds(pl.multiple_of(other_core * half, half), half)], x_old.at[my_rows], xo_send, xo_recv, partner
    )
    for c in o_out:
        c.start()
    x_out.start()

    def piece_of(j):
        return pl.ds(pl.multiple_of(j * COLS, COLS), COLS)

    def to_partner(j):
        piece = x_mid.at[core, pl.ds(0, chip_rows), piece_of(j)]
        return remote_copy(piece, piece, xp_send, xp_recv.at[j], partner)

    def to_across(j):
        src = x_mid.at[core, pl.ds(0, chip_rows), piece_of(j)]
        dst = x_mid.at[core, pl.ds(chip_rows, chip_rows), piece_of(j)]
        return remote_copy(src, dst, xc_send, xc_recv.at[j], across)

    def forward(j):
        piece = x_mid.at[core, pl.ds(chip_rows, chip_rows), pl.ds(j * COLS, COLS)]
        return remote_copy(piece, piece, xf_send, xf_recv.at[j], partner)

    def o_dot(j, k):
        return jnp.dot(o_all[:, o_parts[k]], wo_place(j, k)[...], preferred_element_type=jnp.float32)

    def finish_piece(j, product):
        columns = piece_of(j)
        x_mid[core, pl.ds(0, chip_rows), columns] = (x_old[:, columns].astype(jnp.float32) + product).astype(jnp.bfloat16)
        to_across(j).start()
        to_partner(j).start()

    for c in [x_own] + gains + o_own:
        c.wait()
    for c in [x_out] + o_out:
        c.wait_recv()

    @pl.loop(0, x_pieces)
    def _(j):
        all_bytes(wgu.at[0, pl.ds(0, o_part), pl.ds(0, O_PARTS * COLS)], wo_sem.at[j]).wait()
        finish_piece(j, functools.reduce(jnp.add, [o_dot(j, k) for k in range(O_PARTS)]))

        @pl.when(j == 0)
        def _():
            down_copy(0).start(priority=BULK)

        @pl.when(j == per_region)
        def _():
            down_copy(1).start(priority=BULK)

        for at in range(2):

            @pl.when(j == (at + 1) * per_region - 1)
            def _():
                for i in range(len(steps)):
                    (gate_copy, up_copy)[at](i).start(priority=BULK)

    for n in range(2, d_model // DOWN):
        down_copy(n).start(priority=BULK)

    if next_q:
        q_pairs = q_rsem.shape[0]
        q_width = wq_hbm.shape[2] // (2 * q_pairs)
        spare = d_model - q_width
        over = q_width - spare

        def wq_parts(p):
            region = (wg, wu)[p % 2]
            spans = [(region, 0, 0, q_width)] if p < 2 else [(region, q_width, 0, spare), (wq, (p % 2) * over, spare, over)]
            return [(buffer.at[pl.ds(0, d_model), pl.ds(lane, size)], offset, size) for buffer, lane, offset, size in spans]

        def wq_start(p):
            for place, offset, size in wq_parts(p):
                columns = pl.ds(pl.multiple_of((core * q_pairs + p) * q_width + offset, LANES), size)
                pltpu.make_async_copy(wq_hbm.at[layer + 1, :, columns], place, wq_sem.at[p]).start(priority=BULK)

    def normalize(start):
        window = pl.ds(start, chip_rows)
        halves = [x_mid[h, window, :].astype(jnp.float32) for h in range(2)]
        total = sum(jnp.sum(v * v, axis=-1, keepdims=True) for v in halves)
        factor = lax.rsqrt(total * (1.0 / d_model) + NORM_EPS)
        for h in range(2):
            gain = gain_ref[pl.ds(layer, 1), pl.ds(h * half, half)]
            g_all[window, pl.ds(h * half, half)] = (halves[h] * factor * gain).astype(jnp.bfloat16)

    for j in range(x_pieces):
        to_partner(j).wait_recv()
    normalize(0)
    for j in range(x_pieces):
        to_across(j).wait_recv()
        forward(j).start()
    for j in range(x_pieces):
        forward(j).wait_recv()
    normalize(chip_rows)

    def gate_up(i, start, size):
        window = pl.ds(start, size)
        all_bytes(wgu.at[:, window], w_sem.at[i]).wait()
        dims = (((1,), (1,)), ((), ()))
        gate = lax.dot_general(g_all[...], wg[window, :], dims, preferred_element_type=jnp.float32)
        up = lax.dot_general(g_all[...], wu[window, :], dims, preferred_element_type=jnp.float32)
        a_all[:, window] = (jax.nn.silu(gate) * up).astype(jnp.bfloat16)

    @pl.loop(0, loops)
    def _(t):
        for i in range(loop_steps):
            start, size = steps[i]
            gate_up(t * loop_steps + i, pl.multiple_of(t * SUPER + start, LANES), size)

    for i in range(loops * loop_steps, len(steps)):
        gate_up(i, *steps[i])

    if next_q:
        for p in range(q_pairs):
            wq_start(p)

    def pair_other(n):
        return remote_copy(p_other.at[n, partner_rows], part_in.at[n], p1_send, p1_recv.at[n], partner)

    def cross(n):
        return remote_copy(part_in.at[n], cross_in.at[n], p2_send, p2_recv.at[n], across)

    def pair_own(n):
        return remote_copy(p_own.at[n, partner_rows], own_in.at[n], p3_send, p3_recv.at[n], partner)

    def send_sum(n):
        pair_other(n).wait_recv()
        part_in[n] = p_other[n, my_rows] + part_in[n]
        cross(n).start()

    per_step = DOWN // COLS
    down_steps = d_model // DOWN
    for d in range(down_steps):
        down_copy(d).wait()
    spans = [(0, COLS), (COLS, COLS)] + [(at, DOWN) for at in range(DOWN, d_model, DOWN)]
    given, summed = 0, 0
    for t, (at, size) in enumerate(spans):
        weight = wd[at // DOWN, :, pl.ds(at % DOWN, size)]
        product = jnp.dot(a_all[pl.ds(chip_rows, chip_rows), :], weight, preferred_element_type=jnp.float32)
        ready = 0 if t < 2 else 1 if t == 2 else given
        for e in range(size // COLS):
            p_other[given] = product[:, e * COLS : (e + 1) * COLS]
            pair_other(given).start()
            given += 1
        for n in range(summed, ready):
            send_sum(n)
        summed = max(summed, ready)
    @pl.loop(0, down_steps)
    def _(d):
        @pl.when(d == 0)
        def _():
            for n in range(summed, out_pieces):
                send_sum(n)

        product = jnp.dot(a_all[pl.ds(0, chip_rows), :], wd[d], preferred_element_type=jnp.float32)
        for e in range(per_step):
            n = d * per_step + e
            p_own[n] = product[:, e * COLS : (e + 1) * COLS]
            pair_own(n).start()

    def next_x(n):
        piece = pl.ds(n * COLS, COLS)
        return remote_copy(out_ref.at[:, piece], x_in.at[:, piece], x_send, x_recv.at[n], partner)

    per_half = half // COLS
    for n in range(out_pieces):
        pair_own(n).wait_recv()
        cross(n).wait_recv()
        h, columns = n // per_half, pl.ds((n % per_half) * COLS, COLS)
        total = (p_own[n, my_rows] + own_in[n]) + cross_in[n]
        out_ref[:, pl.ds(n * COLS, COLS)] = (x_mid[h, my_rows, columns].astype(jnp.float32) + total).astype(jnp.bfloat16)
        if next_q:
            next_x(n).start()

    if next_q:
        gain = q_gain_ref[pl.ds(layer + 1, 1), :]
        g_all[pl.ds(0, rows), :] = rms_scaled(out_ref[...], gain)
        for n in range(out_pieces):
            next_x(n).wait_recv()
        g_all[pl.ds(rows, rows), :] = rms_scaled(x_in[...], gain)
        for p in range(q_pairs):
            places = [place for place, _, _ in wq_parts(p)]
            all_bytes(wg.at[pl.ds(0, d_model), pl.ds(0, q_width)], wq_sem.at[p]).wait()
            project_pair(
                p, g_all.at[pl.ds(0, chip_rows)], places, core, q_pairs, q_width // 2, partner,
                q_ref, q_send, q_in, q_ssem, q_rsem,
            )

    x_out.wait_send()
    all_bytes(o_ref, o_send).wait()
    for sem in (xp_send, xc_send, xf_send):
        all_bytes(x_mid.at[0, pl.ds(0, chip_rows)], sem).wait()
    for sem in (p1_send, p2_send, p3_send):
        all_bytes(cross_in, sem).wait()
    if next_q:
        all_bytes(out_ref, x_send).wait()
        receive_pairs(core, q_pairs, partner, q_ref, q_send, q_in, q_ssem, q_rsem)


def tail(layer, o, x, gain, wo, wg_t, wu_t, wd, next_q):
    rows, d_model = x.shape
    hidden = wd.shape[1]
    width = o.shape[1]
    half = d_model // 2
    x_pieces, out_pieces, down_steps = half // COLS, d_model // COLS, d_model // DOWN
    steps = len(hidden_steps(hidden))
    dma = pltpu.SemaphoreType.DMA
    hbm = pl.BlockSpec(memory_space=pltpu.HBM)
    vmem = pl.BlockSpec(memory_space=pltpu.VMEM)
    in_specs = [vmem, hbm, hbm, hbm, hbm, hbm, hbm]
    out_shape = [jax.ShapeDtypeStruct((rows, d_model), jnp.bfloat16)]
    piece = pltpu.VMEM((out_pieces, rows, COLS), jnp.float32)
    scratch = [
        pltpu.VMEM((2 * rows, width), jnp.bfloat16),
        pltpu.VMEM((2 * rows, half), jnp.bfloat16),
        pltpu.VMEM((2, hidden, d_model), jnp.bfloat16),
        pltpu.VMEM((down_steps, hidden, DOWN), jnp.bfloat16),
        pltpu.VMEM((2, 4 * rows, half), jnp.bfloat16),
        pltpu.VMEM((4 * rows, d_model), jnp.bfloat16),
        pltpu.VMEM((4 * rows, hidden), jnp.bfloat16),
        pltpu.VMEM((out_pieces, 2 * rows, COLS), jnp.float32),
        pltpu.VMEM((out_pieces, 2 * rows, COLS), jnp.float32),
        piece, piece, piece, pltpu.VMEM(gain.shape, jnp.float32),
        dma((O_PARTS + 3,)), dma((x_pieces,)), dma((steps,)), dma((down_steps,)),
        dma, dma((O_PARTS,)), dma, dma,
        dma, dma((x_pieces,)), dma, dma((x_pieces,)), dma, dma((x_pieces,)),
        dma, dma((out_pieces,)), dma, dma((out_pieces,)), dma, dma((out_pieces,)),
    ]
    operands = [o, x, gain, wo, wg_t, wu_t, wd]
    if next_q is not None:
        q_gain, wq, heads = next_q
        kv_dim, pairs = wq.shape[2] // heads, heads // 4
        operands += [q_gain, wq]
        in_specs += [hbm, hbm]
        out_shape.append(jax.ShapeDtypeStruct((-(-kv_dim // LANES), heads * rows, LANES), jnp.float32))
        scratch += [
            pltpu.VMEM((d_model, 2 * (4 * kv_dim - d_model)), jnp.bfloat16),
            pltpu.VMEM((pairs, -(-kv_dim // LANES), 2 * rows, LANES), jnp.bfloat16),
            pltpu.VMEM((pairs, -(-kv_dim // LANES), 2 * rows, LANES), jnp.bfloat16),
            pltpu.VMEM((rows, d_model), jnp.bfloat16),
            pltpu.VMEM(q_gain.shape, jnp.float32),
            dma((pairs,)), dma, dma((out_pieces,)), dma, dma((pairs,)),
        ]
    return pl.pallas_call(
        functools.partial(tail_kernel, layer, next_q is not None),
        out_shape=out_shape,
        in_specs=in_specs,
        out_specs=[vmem] * len(out_shape),
        scratch_shapes=scratch,
        compiler_params=pltpu.CompilerParams(collective_id=layer, has_side_effects=True, vmem_limit_bytes=49 * MIB),
        name=f'tail_{layer}',
    )(*operands)


def solution(mesh):
    row_axes = ('replica', 'dp')

    def local_step(x_rows, len_rows, cache, attn_gain, ffn_gain, w_query, w_attn_out, w_up, w_gate, w_down):
        layers, rows, _, kv_dim = cache.shape
        heads = w_query.shape[2] // kv_dim
        latent = w_attn_out.shape[1] // heads
        cache_t = jnp.swapaxes(cache, 2, 3)
        up_t, gate_t = jnp.swapaxes(w_up, 1, 2), jnp.swapaxes(w_gate, 1, 2)
        q = head(pltpu.with_memory_space_constraint(x_rows, pltpu.HBM), pltpu.with_memory_space_constraint(attn_gain, pltpu.HBM), w_query, heads)
        for layer in range(layers):
            mixed = attention(layer, q, len_rows, cache_t, rows, latent)
            next_q = (attn_gain, w_query, heads) if layer + 1 < layers else None
            outs = tail(layer, mixed, x_rows, ffn_gain, w_attn_out, gate_t, up_t, w_down, next_q)
            x_rows, q = outs[0], outs[-1]
        return x_rows

    return jax.shard_map(
        local_step,
        mesh=mesh,
        in_specs=(P(row_axes, None), P(row_axes), P(None, row_axes, None, None), P(), P(), P(), P(),
                  P(None, None, 'dp'), P(None, None, 'dp'), P(None, 'dp', None)),
        out_specs=P(row_axes, None),
        check_vma=False,
    )
```

```python
import functools

import jax
import jax.numpy as jnp
from jax import lax
from jax.experimental import pallas as pl
from jax.experimental.pallas import tpu as pltpu
from jax.sharding import PartitionSpec as P

NORM_EPS = 1e-6
MESH = pl.DeviceIdType.MESH
SEQS = 8
SLOTS = 3
TBLK = 128
PARTS = 2
COLS = 256
HID = 512
DOWN = 512
O_PARTS = 4
MIB = 1024 * 1024
LANES = 128
BULK = 1


def remote_copy(src, dst, send, recv, device):
    return pltpu.make_async_remote_copy(
        src_ref=src, dst_ref=dst, send_sem=send, recv_sem=recv, device_id={'dp': device}, device_id_type=MESH
    )


def all_bytes(ref, sem):
    return pltpu.make_async_copy(ref, ref, sem)


def enter(*peers):
    barrier = pltpu.get_barrier_semaphore()
    for peer in peers:
        pl.semaphore_signal(barrier, inc=1, device_id={'dp': peer}, device_id_type=MESH)
    pl.semaphore_wait(barrier, len(peers))


def hidden_steps(hidden):
    return [(at, min(HID, hidden - at)) for at in range(0, hidden, HID)]


def rms_scaled(rows, gain):
    rows_f = rows.astype(jnp.float32)
    mean_sq = jnp.mean(rows_f * rows_f, axis=-1, keepdims=True)
    return (rows_f * lax.rsqrt(mean_sq + NORM_EPS) * gain).astype(jnp.bfloat16)


def project_pair(p, h_ref, parts, core, pairs, kv_dim, partner, q_ref, q_send, q_in, send_sem, recv_sem):
    rows = q_send.shape[2] // 2
    q = [jnp.dot(h_ref[...], part[...], preferred_element_type=jnp.float32) for part in parts]
    q = q[0] if len(q) == 1 else jnp.concatenate(q, axis=1)
    q = q.astype(jnp.bfloat16)
    for e in range(2):
        own = pl.ds(pl.multiple_of((core * pairs + p) * 2 * rows + e * rows, rows), rows)
        for c in range(q_ref.shape[0]):
            size = min(LANES, kv_dim - c * LANES)
            part = q[:, e * kv_dim + c * LANES :][:, :size]
            q_ref[c, own, pl.ds(0, size)] = part[:rows].astype(jnp.float32)
            q_send[p, c, pl.ds(e * rows, rows), pl.ds(0, size)] = part[rows:]
    remote_copy(q_send.at[p], q_in.at[p], send_sem, recv_sem.at[p], partner).start()


def receive_pairs(core, pairs, partner, q_ref, q_send, q_in, send_sem, recv_sem):
    size = q_send.shape[2]
    for p in range(pairs):
        remote_copy(q_send.at[p], q_in.at[p], send_sem, recv_sem.at[p], partner).wait_recv()
        theirs = pl.ds(pl.multiple_of(((1 - core) * pairs + p) * size, size), size)
        q_ref[:, theirs, :] = q_in[p].astype(jnp.float32)
    all_bytes(q_send, send_sem).wait()


def head_kernel(x_hbm, gain_hbm, wq_hbm, q_ref, x_ref, gain_ref, x_in, h_ref, wq, q_send, q_in, in_sem, wq_sem, x_send, x_recv, q_ssem, q_rsem):
    rows = x_hbm.shape[0]
    width = wq.shape[2]
    pairs = wq.shape[0]
    me = lax.axis_index('dp')
    core = lax.rem(me, 2)
    partner = me + 1 - 2 * core

    def wq_copy(p):
        columns = pl.ds(pl.multiple_of((core * pairs + p) * width, 128), width)
        return pltpu.make_async_copy(wq_hbm.at[0, :, columns], wq.at[p], wq_sem.at[p])

    x_own = pltpu.make_async_copy(x_hbm, x_ref, in_sem.at[0])
    gain_own = pltpu.make_async_copy(gain_hbm, gain_ref, in_sem.at[1])
    x_own.start()
    gain_own.start()
    for p in range(pairs):
        wq_copy(p).start(priority=BULK)
    x_own.wait()
    gain_own.wait()
    enter(partner)
    swap = remote_copy(x_ref, x_in, x_send, x_recv, partner)
    swap.start()
    h_ref[pl.ds(0, rows), :] = rms_scaled(x_ref[...], gain_ref[pl.ds(0, 1), :])
    swap.wait_recv()
    h_ref[pl.ds(rows, rows), :] = rms_scaled(x_in[...], gain_ref[pl.ds(0, 1), :])

    @pl.loop(0, pairs)
    def _(p):
        wq_copy(p).wait()
        project_pair(p, h_ref, [wq.at[p]], core, pairs, width // 2, partner, q_ref, q_send, q_in, q_ssem, q_rsem)

    swap.wait_send()
    receive_pairs(core, pairs, partner, q_ref, q_send, q_in, q_ssem, q_rsem)


def head(x, gain, wq, heads):
    rows, d_model = x.shape
    kv_dim = wq.shape[2] // heads
    pairs = heads // 4
    dma = pltpu.SemaphoreType.DMA
    vmem = pl.BlockSpec(memory_space=pltpu.VMEM)
    return pl.pallas_call(
        head_kernel,
        out_shape=jax.ShapeDtypeStruct((-(-kv_dim // LANES), heads * rows, LANES), jnp.float32),
        in_specs=[pl.BlockSpec(memory_space=pltpu.HBM)] * 3,
        out_specs=vmem,
        scratch_shapes=[
            pltpu.VMEM((rows, d_model), jnp.bfloat16),
            pltpu.VMEM(gain.shape, jnp.float32),
            pltpu.VMEM((rows, d_model), jnp.bfloat16),
            pltpu.VMEM((2 * rows, d_model), jnp.bfloat16),
            pltpu.VMEM((pairs, d_model, 2 * kv_dim), jnp.bfloat16),
            pltpu.VMEM((pairs, -(-kv_dim // LANES), 2 * rows, LANES), jnp.bfloat16),
            pltpu.VMEM((pairs, -(-kv_dim // LANES), 2 * rows, LANES), jnp.bfloat16),
            dma((2,)), dma((pairs,)), dma, dma, dma, dma((pairs,)),
        ],
        compiler_params=pltpu.CompilerParams(collective_id=7, has_side_effects=True, vmem_limit_bytes=48 * MIB),
        name='head',
    )(x, gain, wq)


def attention_kernel(layer, scale, len_ref, q_ref, cache_ref, o_ref, buf, score_buf, prob_buf, o_buf, q_buf, sem):
    rows = o_ref.shape[0]
    heads = q_ref.shape[1] // rows
    kv_dim, seq_len = cache_ref.shape[2:]
    latent = o_ref.shape[1] // heads
    groups = rows // SEQS
    max_blocks = seq_len // TBLK
    split = latent // 2
    dims = (((1,), (1,)), ((), ()))

    def blocks_of(group):
        longest = len_ref[group * SEQS]
        for i in range(1, SEQS):
            longest = jnp.maximum(longest, len_ref[group * SEQS + i])
        return lax.div(longest + (TBLK - 1), TBLK)

    def copy(group, slot, n):
        return pltpu.make_async_copy(
            cache_ref.at[layer, pl.ds(group * SEQS, SEQS), :, pl.ds(0, n * TBLK)],
            buf.at[slot, :, :, pl.ds(0, n * TBLK)],
            sem.at[slot],
        )

    def start(group, slot):
        blocks = blocks_of(group)
        for n in range(1, max_blocks + 1):

            @pl.when(blocks == n)
            def _():
                copy(group, slot, n).start()

    for group in range(min(SLOTS, groups)):
        start(group, group)

    def pack(group):
        out_rows = pl.ds(pl.multiple_of(group * SEQS, SEQS), SEQS)
        for h in range(heads):
            for c in range(latent // LANES):
                source = pl.ds(group * (SEQS * heads) + h, SEQS, stride=heads)
                o_ref[out_rows, pl.ds(h * latent + c * LANES, LANES)] = o_buf[c, source, :].astype(jnp.bfloat16)

    def step(group, carry):
        slot = lax.rem(group, SLOTS)
        blocks = blocks_of(group)
        for n in range(1, max_blocks + 1):

            @pl.when(blocks == n)
            def _():
                copy(group, slot, n).wait()
                width = n * TBLK
                pack(jnp.maximum(group - 1, 0))
                positions = lax.broadcasted_iota(jnp.int32, (heads, width), 1)
                for i in range(SEQS):
                    row = group * SEQS + i
                    query = q_buf[row]
                    score_buf[pl.ds(i * heads, heads), pl.ds(0, width)] = jnp.dot(
                        query, buf[slot, i, :, pl.ds(0, width)], preferred_element_type=jnp.float32
                    )
                for part in range(PARTS):
                    size = SEQS // PARTS
                    for i in range(part * size, (part + 1) * size):
                        row = group * SEQS + i
                        scores = score_buf[pl.ds(i * heads, heads), pl.ds(0, width)]
                        scores = jnp.where(positions < len_ref[row], scores * scale, -jnp.inf)
                        top = jnp.max(scores, axis=-1, keepdims=True)
                        probs = jnp.exp(scores - top)
                        probs = probs * (1.0 / jnp.sum(probs, axis=-1, keepdims=True))
                        prob_buf[pl.ds(i * heads, heads), pl.ds(0, width)] = probs.astype(jnp.bfloat16)
                    for i in range(part * size, (part + 1) * size):
                        row = group * SEQS + i
                        probs = prob_buf[pl.ds(i * heads, heads), pl.ds(0, width)]
                        low = buf[slot, i, pl.ds(0, split), pl.ds(0, width)]
                        high = buf[slot, i, pl.ds(split, latent - split), pl.ds(0, width)]
                        low = lax.dot_general(probs, low, dims, preferred_element_type=jnp.float32)
                        high = lax.dot_general(high, probs, dims, preferred_element_type=jnp.float32)
                        mixed = jnp.concatenate([low, high.T], axis=1)
                        for c in range(latent // LANES):
                            place = pl.ds(pl.multiple_of(row * heads, heads), heads)
                            o_buf[c, place, :] = mixed[:, c * LANES : (c + 1) * LANES]

        @pl.when(group + SLOTS < groups)
        def _():
            start(group + SLOTS, slot)

        return carry

    @pl.loop(0, groups)
    def _(group):
        for i in range(SEQS):
            row = group * SEQS + i
            query = [q_ref[c, pl.ds(row, heads, stride=rows), :] for c in range(q_ref.shape[0])]
            q_buf[row] = jnp.concatenate(query, axis=1)[:, :kv_dim].astype(jnp.bfloat16)

    lax.fori_loop(0, groups, step, 0)
    pack(groups - 1)


def attention(layer, q, lengths, cache_t, rows, latent):
    heads = q.shape[1] // rows
    kv_dim, seq_len = cache_t.shape[2:]
    scale = (3 * (kv_dim - latent)) ** -0.5
    return pl.pallas_call(
        functools.partial(attention_kernel, layer, scale),
        out_shape=jax.ShapeDtypeStruct((rows, heads * latent), jnp.bfloat16),
        in_specs=[
            pl.BlockSpec(memory_space=pltpu.SMEM),
            pl.BlockSpec(memory_space=pltpu.VMEM),
            pl.BlockSpec(memory_space=pl.ANY),
        ],
        out_specs=pl.BlockSpec(memory_space=pltpu.VMEM),
        scratch_shapes=[
            pltpu.VMEM((SLOTS, SEQS, kv_dim, seq_len), jnp.bfloat16),
            pltpu.VMEM((SEQS * heads, seq_len), jnp.float32),
            pltpu.VMEM((SEQS * heads, seq_len), jnp.bfloat16),
            pltpu.VMEM((latent // LANES, rows * heads, LANES), jnp.float32),
            pltpu.VMEM((rows, heads, kv_dim), jnp.bfloat16),
            pltpu.SemaphoreType.DMA((SLOTS,)),
        ],
        compiler_params=pltpu.CompilerParams(vmem_limit_bytes=40 * MIB),
        name=f'attention_{layer}',
    )(lengths, q, cache_t)


def tail_kernel(layer, next_q, *refs):
    refs = list(refs)

    def take(count):
        taken, refs[:count] = refs[:count], []
        return taken

    o_ref, x_hbm, gain_hbm, wo_ref, wg_hbm, wu_hbm, wd_hbm = take(7)
    if next_q:
        q_gain_hbm, wq_hbm = take(2)
    (out_ref,) = take(1)
    if next_q:
        (q_ref,) = take(1)
    o_all, x_old, wgu, wd, x_mid, g_all, a_all, p_other, p_own, part_in, cross_in, own_in, gain_ref = take(13)
    in_sem, wo_sem, w_sem, wd_sem = take(4)
    o_send, o_recv, xo_send, xo_recv, xp_send, xp_recv, xc_send, xc_recv, xf_send, xf_recv = take(10)
    p1_send, p1_recv, p2_send, p2_recv, p3_send, p3_recv = take(6)
    if next_q:
        wq, q_send, q_in, x_in, q_gain_ref, wq_sem, x_send, x_recv, q_ssem, q_rsem = take(10)

    rows, d_model = x_hbm.shape
    chip_rows = 2 * rows
    half = d_model // 2
    hidden = wd_hbm.shape[1]
    o_width = o_ref.shape[1]
    o_part = o_width // O_PARTS
    x_pieces = half // COLS
    out_pieces = d_model // COLS
    steps = hidden_steps(hidden)

    me = lax.axis_index('dp')
    core = lax.rem(me, 2)
    partner = me + 1 - 2 * core
    across = lax.rem(me + 2, 4)
    other_core = 1 - core
    my_rows = pl.ds(pl.multiple_of(core * rows, rows), rows)
    partner_rows = pl.ds(pl.multiple_of(other_core * rows, rows), rows)

    wg, wu = wgu.at[0], wgu.at[1]
    per_region = x_pieces // 2

    def wo_place(j, k):
        lane = pl.multiple_of(lax.rem(j, per_region) * (O_PARTS * COLS) + k * COLS, COLS)
        return wgu.at[lax.div(j, per_region), pl.ds(0, o_part), pl.ds(lane, COLS)]

    def wo_copy(j, k):
        columns = pl.ds(pl.multiple_of(core * half + j * COLS, COLS), COLS)
        return pltpu.make_async_copy(
            wo_ref.at[layer, pl.ds(k * o_part, o_part), columns], wo_place(j, k), wo_sem.at[j]
        )

    def gate_copy(i):
        window = pl.ds(*steps[i])
        return pltpu.make_async_copy(wg_hbm.at[layer, window], wg.at[window], w_sem.at[i])

    def up_copy(i):
        window = pl.ds(*steps[i])
        return pltpu.make_async_copy(wu_hbm.at[layer, window], wu.at[window], w_sem.at[i])

    def down_copy(n):
        columns = pl.ds(n * DOWN, DOWN)
        return pltpu.make_async_copy(wd_hbm.at[layer, :, columns], wd.at[n], wd_sem.at[n])

    o_parts = [pl.ds(k * o_part, o_part) for k in range(O_PARTS)]
    o_own = [pltpu.make_async_copy(o_ref.at[:, w], o_all.at[my_rows, w], in_sem.at[k]) for k, w in enumerate(o_parts)]
    x_own = pltpu.make_async_copy(
        x_hbm.at[:, pl.ds(pl.multiple_of(core * half, half), half)], x_old.at[my_rows], in_sem.at[O_PARTS]
    )
    gains = [pltpu.make_async_copy(gain_hbm, gain_ref, in_sem.at[O_PARTS + 1])]
    if next_q:
        gains.append(pltpu.make_async_copy(q_gain_hbm, q_gain_ref, in_sem.at[O_PARTS + 2]))
    for c in o_own + [x_own] + gains:
        c.start()
    for j in range(x_pieces):
        for k in range(O_PARTS):
            wo_copy(j, k).start(priority=BULK)

    enter(partner, across)

    o_out = [remote_copy(o_ref.at[:, w], o_all.at[my_rows, w], o_send, o_recv.at[k], partner) for k, w in enumerate(o_parts)]
    x_out = remote_copy(
        x_hbm.at[:, pl.ds(pl.multiple_of(other_core * half, half), half)], x_old.at[my_rows], xo_send, xo_recv, partner
    )
    for c in o_out:
        c.start()
    x_out.start()

    def piece_of(j):
        return pl.ds(pl.multiple_of(j * COLS, COLS), COLS)

    def to_partner(j):
        piece = x_mid.at[core, pl.ds(0, chip_rows), piece_of(j)]
        return remote_copy(piece, piece, xp_send, xp_recv.at[j], partner)

    def to_across(j):
        src = x_mid.at[core, pl.ds(0, chip_rows), piece_of(j)]
        dst = x_mid.at[core, pl.ds(chip_rows, chip_rows), piece_of(j)]
        return remote_copy(src, dst, xc_send, xc_recv.at[j], across)

    def forward(j):
        piece = x_mid.at[core, pl.ds(chip_rows, chip_rows), pl.ds(j * COLS, COLS)]
        return remote_copy(piece, piece, xf_send, xf_recv.at[j], partner)

    def o_dot(j, k):
        return jnp.dot(o_all[:, o_parts[k]], wo_place(j, k)[...], preferred_element_type=jnp.float32)

    def finish_piece(j, product):
        columns = piece_of(j)
        x_mid[core, pl.ds(0, chip_rows), columns] = (x_old[:, columns].astype(jnp.float32) + product).astype(jnp.bfloat16)
        to_across(j).start()
        to_partner(j).start()

    for c in [x_own] + gains + o_own:
        c.wait()
    for c in [x_out] + o_out:
        c.wait_recv()

    @pl.loop(0, x_pieces)
    def _(j):
        all_bytes(wgu.at[0, pl.ds(0, o_part), pl.ds(0, O_PARTS * COLS)], wo_sem.at[j]).wait()
        finish_piece(j, functools.reduce(jnp.add, [o_dot(j, k) for k in range(O_PARTS)]))

        @pl.when(j == 0)
        def _():
            down_copy(0).start(priority=BULK)

        @pl.when(j == per_region)
        def _():
            down_copy(1).start(priority=BULK)

        for at in range(2):

            @pl.when(j == (at + 1) * per_region - 1)
            def _():
                for i in range(len(steps)):
                    (gate_copy, up_copy)[at](i).start(priority=BULK)

    for n in range(2, d_model // DOWN):
        down_copy(n).start(priority=BULK)

    if next_q:
        q_pairs = q_rsem.shape[0]
        q_width = wq_hbm.shape[2] // (2 * q_pairs)
        spare = d_model - q_width
        over = q_width - spare

        def wq_parts(p):
            region = (wg, wu)[p % 2]
            spans = [(region, 0, 0, q_width)] if p < 2 else [(region, q_width, 0, spare), (wq, (p % 2) * over, spare, over)]
            return [(buffer.at[pl.ds(0, d_model), pl.ds(lane, size)], offset, size) for buffer, lane, offset, size in spans]

        def wq_start(p):
            for place, offset, size in wq_parts(p):
                columns = pl.ds(pl.multiple_of((core * q_pairs + p) * q_width + offset, LANES), size)
                pltpu.make_async_copy(wq_hbm.at[layer + 1, :, columns], place, wq_sem.at[p]).start(priority=BULK)

    def normalize(start):
        window = pl.ds(start, chip_rows)
        halves = [x_mid[h, window, :].astype(jnp.float32) for h in range(2)]
        total = sum(jnp.sum(v * v, axis=-1, keepdims=True) for v in halves)
        factor = lax.rsqrt(total * (1.0 / d_model) + NORM_EPS)
        for h in range(2):
            gain = gain_ref[pl.ds(layer, 1), pl.ds(h * half, half)]
            g_all[window, pl.ds(h * half, half)] = (halves[h] * factor * gain).astype(jnp.bfloat16)

    for j in range(x_pieces):
        to_partner(j).wait_recv()
    normalize(0)
    for j in range(x_pieces):
        to_across(j).wait_recv()
        forward(j).start()
    for j in range(x_pieces):
        forward(j).wait_recv()
    normalize(chip_rows)

    def gate_up(i, start, size):
        window = pl.ds(start, size)
        all_bytes(wgu.at[:, window], w_sem.at[i]).wait()
        dims = (((1,), (1,)), ((), ()))
        gate = lax.dot_general(g_all[...], wg[window, :], dims, preferred_element_type=jnp.float32)
        up = lax.dot_general(g_all[...], wu[window, :], dims, preferred_element_type=jnp.float32)
        a_all[:, window] = (jax.nn.silu(gate) * up).astype(jnp.bfloat16)

    for i, step in enumerate(steps):
        gate_up(i, *step)

    if next_q:
        for p in range(q_pairs):
            wq_start(p)

    def pair_other(n):
        return remote_copy(p_other.at[n, partner_rows], part_in.at[n], p1_send, p1_recv.at[n], partner)

    def cross(n):
        return remote_copy(part_in.at[n], cross_in.at[n], p2_send, p2_recv.at[n], across)

    def pair_own(n):
        return remote_copy(p_own.at[n, partner_rows], own_in.at[n], p3_send, p3_recv.at[n], partner)

    def send_sum(n):
        pair_other(n).wait_recv()
        part_in[n] = p_other[n, my_rows] + part_in[n]
        cross(n).start()

    per_step = DOWN // COLS
    down_steps = d_model // DOWN
    for d in range(down_steps):
        down_copy(d).wait()
    spans = [(0, COLS), (COLS, DOWN - COLS)] + [(at, DOWN) for at in range(DOWN, d_model, DOWN)]
    given, summed = 0, 0
    for t, (at, size) in enumerate(spans):
        weight = wd[at // DOWN, :, pl.ds(at % DOWN, size)]
        product = jnp.dot(a_all[pl.ds(chip_rows, chip_rows), :], weight, preferred_element_type=jnp.float32)
        ready = 0 if t < 2 else 1 if t == 2 else given
        for e in range(size // COLS):
            p_other[given] = product[:, e * COLS : (e + 1) * COLS]
            pair_other(given).start()
            given += 1
        for n in range(summed, ready):
            send_sum(n)
        summed = max(summed, ready)
    @pl.loop(0, down_steps)
    def _(d):
        @pl.when(d == 0)
        def _():
            for n in range(summed, out_pieces):
                send_sum(n)

        product = jnp.dot(a_all[pl.ds(0, chip_rows), :], wd[d], preferred_element_type=jnp.float32)
        for e in range(per_step):
            n = d * per_step + e
            p_own[n] = product[:, e * COLS : (e + 1) * COLS]
            pair_own(n).start()

    def next_x(n):
        piece = pl.ds(n * COLS, COLS)
        return remote_copy(out_ref.at[:, piece], x_in.at[:, piece], x_send, x_recv.at[n], partner)

    per_half = half // COLS
    for n in range(out_pieces):
        pair_own(n).wait_recv()
        cross(n).wait_recv()
        h, columns = n // per_half, pl.ds((n % per_half) * COLS, COLS)
        total = (p_own[n, my_rows] + own_in[n]) + cross_in[n]
        out_ref[:, pl.ds(n * COLS, COLS)] = (x_mid[h, my_rows, columns].astype(jnp.float32) + total).astype(jnp.bfloat16)
        if next_q:
            next_x(n).start()

    if next_q:
        gain = q_gain_ref[pl.ds(layer + 1, 1), :]
        g_all[pl.ds(0, rows), :] = rms_scaled(out_ref[...], gain)
        for n in range(out_pieces):
            next_x(n).wait_recv()
        g_all[pl.ds(rows, rows), :] = rms_scaled(x_in[...], gain)
        for p in range(q_pairs):
            places = [place for place, _, _ in wq_parts(p)]
            all_bytes(wg.at[pl.ds(0, d_model), pl.ds(0, q_width)], wq_sem.at[p]).wait()
            project_pair(
                p, g_all.at[pl.ds(0, chip_rows)], places, core, q_pairs, q_width // 2, partner,
                q_ref, q_send, q_in, q_ssem, q_rsem,
            )

    x_out.wait_send()
    all_bytes(o_ref, o_send).wait()
    for sem in (xp_send, xc_send, xf_send):
        all_bytes(x_mid.at[0, pl.ds(0, chip_rows)], sem).wait()
    for sem in (p1_send, p2_send, p3_send):
        all_bytes(cross_in, sem).wait()
    if next_q:
        all_bytes(out_ref, x_send).wait()
        receive_pairs(core, q_pairs, partner, q_ref, q_send, q_in, q_ssem, q_rsem)


def tail(layer, o, x, gain, wo, wg_t, wu_t, wd, next_q):
    rows, d_model = x.shape
    hidden = wd.shape[1]
    width = o.shape[1]
    half = d_model // 2
    x_pieces, out_pieces, down_steps = half // COLS, d_model // COLS, d_model // DOWN
    steps = len(hidden_steps(hidden))
    dma = pltpu.SemaphoreType.DMA
    hbm = pl.BlockSpec(memory_space=pltpu.HBM)
    vmem = pl.BlockSpec(memory_space=pltpu.VMEM)
    in_specs = [vmem, hbm, hbm, hbm, hbm, hbm, hbm]
    out_shape = [jax.ShapeDtypeStruct((rows, d_model), jnp.bfloat16)]
    piece = pltpu.VMEM((out_pieces, rows, COLS), jnp.float32)
    scratch = [
        pltpu.VMEM((2 * rows, width), jnp.bfloat16),
        pltpu.VMEM((2 * rows, half), jnp.bfloat16),
        pltpu.VMEM((2, hidden, d_model), jnp.bfloat16),
        pltpu.VMEM((down_steps, hidden, DOWN), jnp.bfloat16),
        pltpu.VMEM((2, 4 * rows, half), jnp.bfloat16),
        pltpu.VMEM((4 * rows, d_model), jnp.bfloat16),
        pltpu.VMEM((4 * rows, hidden), jnp.bfloat16),
        pltpu.VMEM((out_pieces, 2 * rows, COLS), jnp.float32),
        pltpu.VMEM((out_pieces, 2 * rows, COLS), jnp.float32),
        piece, piece, piece, pltpu.VMEM(gain.shape, jnp.float32),
        dma((O_PARTS + 3,)), dma((x_pieces,)), dma((steps,)), dma((down_steps,)),
        dma, dma((O_PARTS,)), dma, dma,
        dma, dma((x_pieces,)), dma, dma((x_pieces,)), dma, dma((x_pieces,)),
        dma, dma((out_pieces,)), dma, dma((out_pieces,)), dma, dma((out_pieces,)),
    ]
    operands = [o, x, gain, wo, wg_t, wu_t, wd]
    if next_q is not None:
        q_gain, wq, heads = next_q
        kv_dim, pairs = wq.shape[2] // heads, heads // 4
        operands += [q_gain, wq]
        in_specs += [hbm, hbm]
        out_shape.append(jax.ShapeDtypeStruct((-(-kv_dim // LANES), heads * rows, LANES), jnp.float32))
        scratch += [
            pltpu.VMEM((d_model, 2 * (4 * kv_dim - d_model)), jnp.bfloat16),
            pltpu.VMEM((pairs, -(-kv_dim // LANES), 2 * rows, LANES), jnp.bfloat16),
            pltpu.VMEM((pairs, -(-kv_dim // LANES), 2 * rows, LANES), jnp.bfloat16),
            pltpu.VMEM((rows, d_model), jnp.bfloat16),
            pltpu.VMEM(q_gain.shape, jnp.float32),
            dma((pairs,)), dma, dma((out_pieces,)), dma, dma((pairs,)),
        ]
    return pl.pallas_call(
        functools.partial(tail_kernel, layer, next_q is not None),
        out_shape=out_shape,
        in_specs=in_specs,
        out_specs=[vmem] * len(out_shape),
        scratch_shapes=scratch,
        compiler_params=pltpu.CompilerParams(collective_id=layer, has_side_effects=True, vmem_limit_bytes=49 * MIB),
        name=f'tail_{layer}',
    )(*operands)


def solution(mesh):
    row_axes = ('replica', 'dp')

    def local_step(x_rows, len_rows, cache, attn_gain, ffn_gain, w_query, w_attn_out, w_up, w_gate, w_down):
        layers, rows, _, kv_dim = cache.shape
        heads = w_query.shape[2] // kv_dim
        latent = w_attn_out.shape[1] // heads
        cache_t = jnp.swapaxes(cache, 2, 3)
        up_t, gate_t = jnp.swapaxes(w_up, 1, 2), jnp.swapaxes(w_gate, 1, 2)
        q = head(pltpu.with_memory_space_constraint(x_rows, pltpu.HBM), pltpu.with_memory_space_constraint(attn_gain, pltpu.HBM), w_query, heads)
        for layer in range(layers):
            mixed = attention(layer, q, len_rows, cache_t, rows, latent)
            next_q = (attn_gain, w_query, heads) if layer + 1 < layers else None
            outs = tail(layer, mixed, x_rows, ffn_gain, w_attn_out, gate_t, up_t, w_down, next_q)
            x_rows, q = outs[0], outs[-1]
        return x_rows

    return jax.shard_map(
        local_step,
        mesh=mesh,
        in_specs=(P(row_axes, None), P(row_axes), P(None, row_axes, None, None), P(), P(), P(), P(),
                  P(None, None, 'dp'), P(None, None, 'dp'), P(None, 'dp', None)),
        out_specs=P(row_axes, None),
        check_vma=False,
    )
```

```python
import functools

import jax
import jax.numpy as jnp
from jax import lax
from jax.experimental import pallas as pl
from jax.experimental.pallas import tpu as pltpu
from jax.sharding import PartitionSpec as P

NORM_EPS = 1e-6
MESH = pl.DeviceIdType.MESH
SEQS = 8
SLOTS = 3
TBLK = 128
PARTS = 2
COLS = 256
HID = 512
DOWN = 512
O_PARTS = 4
MIB = 1024 * 1024
LANES = 128
BULK = 1


def remote_copy(src, dst, send, recv, device):
    return pltpu.make_async_remote_copy(
        src_ref=src, dst_ref=dst, send_sem=send, recv_sem=recv, device_id={'dp': device}, device_id_type=MESH
    )


def all_bytes(ref, sem):
    return pltpu.make_async_copy(ref, ref, sem)


def enter(*peers):
    barrier = pltpu.get_barrier_semaphore()
    for peer in peers:
        pl.semaphore_signal(barrier, inc=1, device_id={'dp': peer}, device_id_type=MESH)
    pl.semaphore_wait(barrier, len(peers))


def hidden_steps(hidden):
    return [(at, min(HID, hidden - at)) for at in range(0, hidden, HID)]


def rms_scaled(rows, gain):
    rows_f = rows.astype(jnp.float32)
    mean_sq = jnp.mean(rows_f * rows_f, axis=-1, keepdims=True)
    return (rows_f * lax.rsqrt(mean_sq + NORM_EPS) * gain).astype(jnp.bfloat16)


def project_pair(p, h_ref, parts, core, pairs, kv_dim, partner, q_ref, q_send, q_in, send_sem, recv_sem):
    rows = q_send.shape[2] // 2
    q = [jnp.dot(h_ref[...], part[...], preferred_element_type=jnp.float32) for part in parts]
    q = q[0] if len(q) == 1 else jnp.concatenate(q, axis=1)
    q = q.astype(jnp.bfloat16)
    for e in range(2):
        own = pl.ds(pl.multiple_of((core * pairs + p) * 2 * rows + e * rows, rows), rows)
        for c in range(q_ref.shape[0]):
            size = min(LANES, kv_dim - c * LANES)
            part = q[:, e * kv_dim + c * LANES :][:, :size]
            q_ref[c, own, pl.ds(0, size)] = part[:rows].astype(jnp.float32)
            q_send[p, c, pl.ds(e * rows, rows), pl.ds(0, size)] = part[rows:]
    remote_copy(q_send.at[p], q_in.at[p], send_sem, recv_sem.at[p], partner).start()


def receive_pairs(core, pairs, partner, q_ref, q_send, q_in, send_sem, recv_sem):
    size = q_send.shape[2]
    for p in range(pairs):
        remote_copy(q_send.at[p], q_in.at[p], send_sem, recv_sem.at[p], partner).wait_recv()
        theirs = pl.ds(pl.multiple_of(((1 - core) * pairs + p) * size, size), size)
        q_ref[:, theirs, :] = q_in[p].astype(jnp.float32)
    all_bytes(q_send, send_sem).wait()


def head_kernel(x_hbm, gain_hbm, wq_hbm, q_ref, x_ref, gain_ref, x_in, h_ref, wq, q_send, q_in, in_sem, wq_sem, x_send, x_recv, q_ssem, q_rsem):
    rows = x_hbm.shape[0]
    width = wq.shape[2]
    pairs = wq.shape[0]
    me = lax.axis_index('dp')
    core = lax.rem(me, 2)
    partner = me + 1 - 2 * core

    def wq_copy(p):
        columns = pl.ds(pl.multiple_of((core * pairs + p) * width, 128), width)
        return pltpu.make_async_copy(wq_hbm.at[0, :, columns], wq.at[p], wq_sem.at[p])

    x_own = pltpu.make_async_copy(x_hbm, x_ref, in_sem.at[0])
    gain_own = pltpu.make_async_copy(gain_hbm, gain_ref, in_sem.at[1])
    x_own.start()
    gain_own.start()
    for p in range(pairs):
        wq_copy(p).start(priority=BULK)
    x_own.wait()
    gain_own.wait()
    enter(partner)
    swap = remote_copy(x_ref, x_in, x_send, x_recv, partner)
    swap.start()
    h_ref[pl.ds(0, rows), :] = rms_scaled(x_ref[...], gain_ref[pl.ds(0, 1), :])
    swap.wait_recv()
    h_ref[pl.ds(rows, rows), :] = rms_scaled(x_in[...], gain_ref[pl.ds(0, 1), :])

    @pl.loop(0, pairs)
    def _(p):
        wq_copy(p).wait()
        project_pair(p, h_ref, [wq.at[p]], core, pairs, width // 2, partner, q_ref, q_send, q_in, q_ssem, q_rsem)

    swap.wait_send()
    receive_pairs(core, pairs, partner, q_ref, q_send, q_in, q_ssem, q_rsem)


def head(x, gain, wq, heads):
    rows, d_model = x.shape
    kv_dim = wq.shape[2] // heads
    pairs = heads // 4
    dma = pltpu.SemaphoreType.DMA
    vmem = pl.BlockSpec(memory_space=pltpu.VMEM)
    return pl.pallas_call(
        head_kernel,
        out_shape=jax.ShapeDtypeStruct((-(-kv_dim // LANES), heads * rows, LANES), jnp.float32),
        in_specs=[pl.BlockSpec(memory_space=pltpu.HBM)] * 3,
        out_specs=vmem,
        scratch_shapes=[
            pltpu.VMEM((rows, d_model), jnp.bfloat16),
            pltpu.VMEM(gain.shape, jnp.float32),
            pltpu.VMEM((rows, d_model), jnp.bfloat16),
            pltpu.VMEM((2 * rows, d_model), jnp.bfloat16),
            pltpu.VMEM((pairs, d_model, 2 * kv_dim), jnp.bfloat16),
            pltpu.VMEM((pairs, -(-kv_dim // LANES), 2 * rows, LANES), jnp.bfloat16),
            pltpu.VMEM((pairs, -(-kv_dim // LANES), 2 * rows, LANES), jnp.bfloat16),
            dma((2,)), dma((pairs,)), dma, dma, dma, dma((pairs,)),
        ],
        compiler_params=pltpu.CompilerParams(collective_id=7, has_side_effects=True, vmem_limit_bytes=48 * MIB),
        name='head',
    )(x, gain, wq)


def attention_kernel(layer, scale, len_ref, q_ref, cache_ref, o_ref, buf, score_buf, prob_buf, o_buf, q_buf, sem):
    rows = o_ref.shape[0]
    heads = q_ref.shape[1] // rows
    kv_dim, seq_len = cache_ref.shape[2:]
    latent = o_ref.shape[1] // heads
    groups = rows // SEQS
    max_blocks = seq_len // TBLK
    split = latent // 2
    dims = (((1,), (1,)), ((), ()))

    def blocks_of(group):
        longest = len_ref[group * SEQS]
        for i in range(1, SEQS):
            longest = jnp.maximum(longest, len_ref[group * SEQS + i])
        return lax.div(longest + (TBLK - 1), TBLK)

    def copy(group, slot, n):
        return pltpu.make_async_copy(
            cache_ref.at[layer, pl.ds(group * SEQS, SEQS), :, pl.ds(0, n * TBLK)],
            buf.at[slot, :, :, pl.ds(0, n * TBLK)],
            sem.at[slot],
        )

    def start(group, slot):
        blocks = blocks_of(group)
        for n in range(1, max_blocks + 1):

            @pl.when(blocks == n)
            def _():
                copy(group, slot, n).start()

    for group in range(min(SLOTS, groups)):
        start(group, group)

    def pack(group):
        out_rows = pl.ds(pl.multiple_of(group * SEQS, SEQS), SEQS)
        for h in range(heads):
            for c in range(latent // LANES):
                source = pl.ds(group * (SEQS * heads) + h, SEQS, stride=heads)
                o_ref[out_rows, pl.ds(h * latent + c * LANES, LANES)] = o_buf[c, source, :].astype(jnp.bfloat16)

    def step(group, carry):
        slot = lax.rem(group, SLOTS)
        blocks = blocks_of(group)
        for n in range(1, max_blocks + 1):

            @pl.when(blocks == n)
            def _():
                copy(group, slot, n).wait()
                width = n * TBLK
                pack(jnp.maximum(group - 1, 0))
                positions = lax.broadcasted_iota(jnp.int32, (heads, width), 1)
                for i in range(SEQS):
                    row = group * SEQS + i
                    query = q_buf[row]
                    score_buf[pl.ds(i * heads, heads), pl.ds(0, width)] = jnp.dot(
                        query, buf[slot, i, :, pl.ds(0, width)], preferred_element_type=jnp.float32
                    )
                for part in range(PARTS):
                    size = SEQS // PARTS
                    for i in range(part * size, (part + 1) * size):
                        row = group * SEQS + i
                        scores = score_buf[pl.ds(i * heads, heads), pl.ds(0, width)]
                        scores = jnp.where(positions < len_ref[row], scores * scale, -jnp.inf)
                        top = jnp.max(scores, axis=-1, keepdims=True)
                        probs = jnp.exp(scores - top)
                        probs = probs * (1.0 / jnp.sum(probs, axis=-1, keepdims=True))
                        prob_buf[pl.ds(i * heads, heads), pl.ds(0, width)] = probs.astype(jnp.bfloat16)
                    for i in range(part * size, (part + 1) * size):
                        row = group * SEQS + i
                        probs = prob_buf[pl.ds(i * heads, heads), pl.ds(0, width)]
                        low = buf[slot, i, pl.ds(0, split), pl.ds(0, width)]
                        high = buf[slot, i, pl.ds(split, latent - split), pl.ds(0, width)]
                        low = lax.dot_general(probs, low, dims, preferred_element_type=jnp.float32)
                        high = lax.dot_general(high, probs, dims, preferred_element_type=jnp.float32)
                        mixed = jnp.concatenate([low, high.T], axis=1)
                        for c in range(latent // LANES):
                            place = pl.ds(pl.multiple_of(row * heads, heads), heads)
                            o_buf[c, place, :] = mixed[:, c * LANES : (c + 1) * LANES]

        @pl.when(group + SLOTS < groups)
        def _():
            start(group + SLOTS, slot)

        return carry

    @pl.loop(0, groups)
    def _(group):
        for i in range(SEQS):
            row = group * SEQS + i
            query = [q_ref[c, pl.ds(row, heads, stride=rows), :] for c in range(q_ref.shape[0])]
            q_buf[row] = jnp.concatenate(query, axis=1)[:, :kv_dim].astype(jnp.bfloat16)

    lax.fori_loop(0, groups, step, 0)
    pack(groups - 1)


def attention(layer, q, lengths, cache_t, rows, latent):
    heads = q.shape[1] // rows
    kv_dim, seq_len = cache_t.shape[2:]
    scale = (3 * (kv_dim - latent)) ** -0.5
    return pl.pallas_call(
        functools.partial(attention_kernel, layer, scale),
        out_shape=jax.ShapeDtypeStruct((rows, heads * latent), jnp.bfloat16),
        in_specs=[
            pl.BlockSpec(memory_space=pltpu.SMEM),
            pl.BlockSpec(memory_space=pltpu.VMEM),
            pl.BlockSpec(memory_space=pl.ANY),
        ],
        out_specs=pl.BlockSpec(memory_space=pltpu.VMEM),
        scratch_shapes=[
            pltpu.VMEM((SLOTS, SEQS, kv_dim, seq_len), jnp.bfloat16),
            pltpu.VMEM((SEQS * heads, seq_len), jnp.float32),
            pltpu.VMEM((SEQS * heads, seq_len), jnp.bfloat16),
            pltpu.VMEM((latent // LANES, rows * heads, LANES), jnp.float32),
            pltpu.VMEM((rows, heads, kv_dim), jnp.bfloat16),
            pltpu.SemaphoreType.DMA((SLOTS,)),
        ],
        compiler_params=pltpu.CompilerParams(vmem_limit_bytes=40 * MIB),
        name=f'attention_{layer}',
    )(lengths, q, cache_t)


def tail_kernel(layer, next_q, *refs):
    refs = list(refs)

    def take(count):
        taken, refs[:count] = refs[:count], []
        return taken

    o_ref, x_hbm, gain_hbm, wo_ref, wg_hbm, wu_hbm, wd_hbm = take(7)
    if next_q:
        q_gain_hbm, wq_hbm = take(2)
    (out_ref,) = take(1)
    if next_q:
        (q_ref,) = take(1)
    o_all, x_old, wgu, wd, x_mid, g_all, a_all, p_other, p_own, part_in, cross_in, own_in, gain_ref = take(13)
    in_sem, wo_sem, w_sem, wd_sem = take(4)
    o_send, o_recv, xo_send, xo_recv, xp_send, xp_recv, xc_send, xc_recv, xf_send, xf_recv = take(10)
    p1_send, p1_recv, p2_send, p2_recv, p3_send, p3_recv = take(6)
    if next_q:
        wq, q_send, q_in, x_in, q_gain_ref, wq_sem, x_send, x_recv, q_ssem, q_rsem = take(10)

    rows, d_model = x_hbm.shape
    chip_rows = 2 * rows
    half = d_model // 2
    hidden = wd_hbm.shape[1]
    o_width = o_ref.shape[1]
    o_part = o_width // O_PARTS
    x_pieces = half // COLS
    out_pieces = d_model // COLS
    steps = hidden_steps(hidden)

    me = lax.axis_index('dp')
    core = lax.rem(me, 2)
    partner = me + 1 - 2 * core
    across = lax.rem(me + 2, 4)
    other_core = 1 - core
    my_rows = pl.ds(pl.multiple_of(core * rows, rows), rows)
    partner_rows = pl.ds(pl.multiple_of(other_core * rows, rows), rows)

    wg, wu = wgu.at[0], wgu.at[1]
    per_region = x_pieces // 2

    def wo_place(j, k):
        lane = pl.multiple_of(lax.rem(j, per_region) * (O_PARTS * COLS) + k * COLS, COLS)
        return wgu.at[lax.div(j, per_region), pl.ds(0, o_part), pl.ds(lane, COLS)]

    def wo_copy(j, k):
        columns = pl.ds(pl.multiple_of(core * half + j * COLS, COLS), COLS)
        return pltpu.make_async_copy(
            wo_ref.at[layer, pl.ds(k * o_part, o_part), columns], wo_place(j, k), wo_sem.at[j]
        )

    def gate_copy(i):
        window = pl.ds(*steps[i])
        return pltpu.make_async_copy(wg_hbm.at[layer, window], wg.at[window], w_sem.at[i])

    def up_copy(i):
        window = pl.ds(*steps[i])
        return pltpu.make_async_copy(wu_hbm.at[layer, window], wu.at[window], w_sem.at[i])

    def down_copy(n):
        columns = pl.ds(n * DOWN, DOWN)
        return pltpu.make_async_copy(wd_hbm.at[layer, :, columns], wd.at[n], wd_sem.at[n])

    o_parts = [pl.ds(k * o_part, o_part) for k in range(O_PARTS)]
    x_own = pltpu.make_async_copy(
        x_hbm.at[:, pl.ds(pl.multiple_of(core * half, half), half)], x_old.at[my_rows], in_sem.at[0]
    )
    gains = [pltpu.make_async_copy(gain_hbm, gain_ref, in_sem.at[1])]
    if next_q:
        gains.append(pltpu.make_async_copy(q_gain_hbm, q_gain_ref, in_sem.at[2]))
    for c in [x_own] + gains:
        c.start()
    for j in range(x_pieces):
        for k in range(O_PARTS):
            wo_copy(j, k).start(priority=BULK)

    enter(partner, across)

    o_out = [remote_copy(o_ref.at[:, w], o_all.at[my_rows, w], o_send, o_recv.at[k], partner) for k, w in enumerate(o_parts)]
    x_out = remote_copy(
        x_hbm.at[:, pl.ds(pl.multiple_of(other_core * half, half), half)], x_old.at[my_rows], xo_send, xo_recv, partner
    )
    for c in o_out:
        c.start()
    x_out.start()

    def piece_of(j):
        return pl.ds(pl.multiple_of(j * COLS, COLS), COLS)

    def to_partner(j):
        piece = x_mid.at[core, pl.ds(0, chip_rows), piece_of(j)]
        return remote_copy(piece, piece, xp_send, xp_recv.at[j], partner)

    def to_across(j):
        src = x_mid.at[core, pl.ds(0, chip_rows), piece_of(j)]
        dst = x_mid.at[core, pl.ds(chip_rows, chip_rows), piece_of(j)]
        return remote_copy(src, dst, xc_send, xc_recv.at[j], across)

    def forward(j):
        piece = x_mid.at[core, pl.ds(chip_rows, chip_rows), pl.ds(j * COLS, COLS)]
        return remote_copy(piece, piece, xf_send, xf_recv.at[j], partner)

    def o_dot(j, k):
        return jnp.dot(o_all[:, o_parts[k]], wo_place(j, k)[...], preferred_element_type=jnp.float32)

    def finish_piece(j, product):
        columns = piece_of(j)
        x_mid[core, pl.ds(0, chip_rows), columns] = (x_old[:, columns].astype(jnp.float32) + product).astype(jnp.bfloat16)
        to_across(j).start()
        to_partner(j).start()

    o_all[my_rows, :] = o_ref[...]
    for c in [x_own] + gains:
        c.wait()
    for c in [x_out] + o_out:
        c.wait_recv()

    @pl.loop(0, x_pieces)
    def _(j):
        all_bytes(wgu.at[0, pl.ds(0, o_part), pl.ds(0, O_PARTS * COLS)], wo_sem.at[j]).wait()
        finish_piece(j, functools.reduce(jnp.add, [o_dot(j, k) for k in range(O_PARTS)]))

        @pl.when(j == 0)
        def _():
            down_copy(0).start(priority=BULK)

        @pl.when(j == per_region)
        def _():
            down_copy(1).start(priority=BULK)

        for at in range(2):

            @pl.when(j == (at + 1) * per_region - 1)
            def _():
                for i in range(len(steps)):
                    (gate_copy, up_copy)[at](i).start(priority=BULK)

    for n in range(2, d_model // DOWN):
        down_copy(n).start(priority=BULK)

    if next_q:
        q_pairs = q_rsem.shape[0]
        q_width = wq_hbm.shape[2] // (2 * q_pairs)
        spare = d_model - q_width
        over = q_width - spare

        def wq_parts(p):
            region = (wg, wu)[p % 2]
            spans = [(region, 0, 0, q_width)] if p < 2 else [(region, q_width, 0, spare), (wq, (p % 2) * over, spare, over)]
            return [(buffer.at[pl.ds(0, d_model), pl.ds(lane, size)], offset, size) for buffer, lane, offset, size in spans]

        def wq_start(p):
            for place, offset, size in wq_parts(p):
                columns = pl.ds(pl.multiple_of((core * q_pairs + p) * q_width + offset, LANES), size)
                pltpu.make_async_copy(wq_hbm.at[layer + 1, :, columns], place, wq_sem.at[p]).start(priority=BULK)

    def normalize(start):
        window = pl.ds(start, chip_rows)
        halves = [x_mid[h, window, :].astype(jnp.float32) for h in range(2)]
        total = sum(jnp.sum(v * v, axis=-1, keepdims=True) for v in halves)
        factor = lax.rsqrt(total * (1.0 / d_model) + NORM_EPS)
        for h in range(2):
            gain = gain_ref[pl.ds(layer, 1), pl.ds(h * half, half)]
            g_all[window, pl.ds(h * half, half)] = (halves[h] * factor * gain).astype(jnp.bfloat16)

    for j in range(x_pieces):
        to_partner(j).wait_recv()
    normalize(0)
    for j in range(x_pieces):
        to_across(j).wait_recv()
        forward(j).start()
    for j in range(x_pieces):
        forward(j).wait_recv()
    normalize(chip_rows)

    def gate_up(i, start, size):
        window = pl.ds(start, size)
        all_bytes(wgu.at[:, window], w_sem.at[i]).wait()
        dims = (((1,), (1,)), ((), ()))
        gate = lax.dot_general(g_all[...], wg[window, :], dims, preferred_element_type=jnp.float32)
        up = lax.dot_general(g_all[...], wu[window, :], dims, preferred_element_type=jnp.float32)
        a_all[:, window] = (jax.nn.silu(gate) * up).astype(jnp.bfloat16)

    for i, step in enumerate(steps):
        gate_up(i, *step)

    if next_q:
        for p in range(q_pairs):
            wq_start(p)

    def pair_other(n):
        return remote_copy(p_other.at[n, partner_rows], part_in.at[n], p1_send, p1_recv.at[n], partner)

    def cross(n):
        return remote_copy(part_in.at[n], cross_in.at[n], p2_send, p2_recv.at[n], across)

    def pair_own(n):
        return remote_copy(p_own.at[n, partner_rows], own_in.at[n], p3_send, p3_recv.at[n], partner)

    def send_sum(n):
        pair_other(n).wait_recv()
        part_in[n] = p_other[n, my_rows] + part_in[n]
        cross(n).start()

    per_step = DOWN // COLS
    down_steps = d_model // DOWN
    for d in range(down_steps):
        down_copy(d).wait()
    spans = [(0, COLS), (COLS, DOWN - COLS)] + [(at, DOWN) for at in range(DOWN, d_model, DOWN)]
    given, summed = 0, 0
    for t, (at, size) in enumerate(spans):
        weight = wd[at // DOWN, :, pl.ds(at % DOWN, size)]
        product = jnp.dot(a_all[pl.ds(chip_rows, chip_rows), :], weight, preferred_element_type=jnp.float32)
        ready = 0 if t < 2 else 1 if t == 2 else given
        for e in range(size // COLS):
            p_other[given] = product[:, e * COLS : (e + 1) * COLS]
            pair_other(given).start()
            given += 1
        for n in range(summed, ready):
            send_sum(n)
        summed = max(summed, ready)
    @pl.loop(0, down_steps)
    def _(d):
        @pl.when(d == 0)
        def _():
            for n in range(summed, out_pieces):
                send_sum(n)

        product = jnp.dot(a_all[pl.ds(0, chip_rows), :], wd[d], preferred_element_type=jnp.float32)
        for e in range(per_step):
            n = d * per_step + e
            p_own[n] = product[:, e * COLS : (e + 1) * COLS]
            pair_own(n).start()

    def next_x(n):
        piece = pl.ds(n * COLS, COLS)
        return remote_copy(out_ref.at[:, piece], x_in.at[:, piece], x_send, x_recv.at[n], partner)

    per_half = half // COLS
    for n in range(out_pieces):
        pair_own(n).wait_recv()
        cross(n).wait_recv()
        h, columns = n // per_half, pl.ds((n % per_half) * COLS, COLS)
        total = (p_own[n, my_rows] + own_in[n]) + cross_in[n]
        out_ref[:, pl.ds(n * COLS, COLS)] = (x_mid[h, my_rows, columns].astype(jnp.float32) + total).astype(jnp.bfloat16)
        if next_q:
            next_x(n).start()

    if next_q:
        gain = q_gain_ref[pl.ds(layer + 1, 1), :]
        g_all[pl.ds(0, rows), :] = rms_scaled(out_ref[...], gain)
        for n in range(out_pieces):
            next_x(n).wait_recv()
        g_all[pl.ds(rows, rows), :] = rms_scaled(x_in[...], gain)
        for p in range(q_pairs):
            places = [place for place, _, _ in wq_parts(p)]
            all_bytes(wg.at[pl.ds(0, d_model), pl.ds(0, q_width)], wq_sem.at[p]).wait()
            project_pair(
                p, g_all.at[pl.ds(0, chip_rows)], places, core, q_pairs, q_width // 2, partner,
                q_ref, q_send, q_in, q_ssem, q_rsem,
            )

    x_out.wait_send()
    all_bytes(o_ref, o_send).wait()
    for sem in (xp_send, xc_send, xf_send):
        all_bytes(x_mid.at[0, pl.ds(0, chip_rows)], sem).wait()
    for sem in (p1_send, p2_send, p3_send):
        all_bytes(cross_in, sem).wait()
    if next_q:
        all_bytes(out_ref, x_send).wait()
        receive_pairs(core, q_pairs, partner, q_ref, q_send, q_in, q_ssem, q_rsem)


def tail(layer, o, x, gain, wo, wg_t, wu_t, wd, next_q):
    rows, d_model = x.shape
    hidden = wd.shape[1]
    width = o.shape[1]
    half = d_model // 2
    x_pieces, out_pieces, down_steps = half // COLS, d_model // COLS, d_model // DOWN
    steps = len(hidden_steps(hidden))
    dma = pltpu.SemaphoreType.DMA
    hbm = pl.BlockSpec(memory_space=pltpu.HBM)
    vmem = pl.BlockSpec(memory_space=pltpu.VMEM)
    in_specs = [vmem, hbm, hbm, hbm, hbm, hbm, hbm]
    out_shape = [jax.ShapeDtypeStruct((rows, d_model), jnp.bfloat16)]
    piece = pltpu.VMEM((out_pieces, rows, COLS), jnp.float32)
    scratch = [
        pltpu.VMEM((2 * rows, width), jnp.bfloat16),
        pltpu.VMEM((2 * rows, half), jnp.bfloat16),
        pltpu.VMEM((2, hidden, d_model), jnp.bfloat16),
        pltpu.VMEM((down_steps, hidden, DOWN), jnp.bfloat16),
        pltpu.VMEM((2, 4 * rows, half), jnp.bfloat16),
        pltpu.VMEM((4 * rows, d_model), jnp.bfloat16),
        pltpu.VMEM((4 * rows, hidden), jnp.bfloat16),
        pltpu.VMEM((out_pieces, 2 * rows, COLS), jnp.float32),
        pltpu.VMEM((out_pieces, 2 * rows, COLS), jnp.float32),
        piece, piece, piece, pltpu.VMEM(gain.shape, jnp.float32),
        dma((3,)), dma((x_pieces,)), dma((steps,)), dma((down_steps,)),
        dma, dma((O_PARTS,)), dma, dma,
        dma, dma((x_pieces,)), dma, dma((x_pieces,)), dma, dma((x_pieces,)),
        dma, dma((out_pieces,)), dma, dma((out_pieces,)), dma, dma((out_pieces,)),
    ]
    operands = [o, x, gain, wo, wg_t, wu_t, wd]
    if next_q is not None:
        q_gain, wq, heads = next_q
        kv_dim, pairs = wq.shape[2] // heads, heads // 4
        operands += [q_gain, wq]
        in_specs += [hbm, hbm]
        out_shape.append(jax.ShapeDtypeStruct((-(-kv_dim // LANES), heads * rows, LANES), jnp.float32))
        scratch += [
            pltpu.VMEM((d_model, 2 * (4 * kv_dim - d_model)), jnp.bfloat16),
            pltpu.VMEM((pairs, -(-kv_dim // LANES), 2 * rows, LANES), jnp.bfloat16),
            pltpu.VMEM((pairs, -(-kv_dim // LANES), 2 * rows, LANES), jnp.bfloat16),
            pltpu.VMEM((rows, d_model), jnp.bfloat16),
            pltpu.VMEM(q_gain.shape, jnp.float32),
            dma((pairs,)), dma, dma((out_pieces,)), dma, dma((pairs,)),
        ]
    return pl.pallas_call(
        functools.partial(tail_kernel, layer, next_q is not None),
        out_shape=out_shape,
        in_specs=in_specs,
        out_specs=[vmem] * len(out_shape),
        scratch_shapes=scratch,
        compiler_params=pltpu.CompilerParams(collective_id=layer, has_side_effects=True, vmem_limit_bytes=49 * MIB),
        name=f'tail_{layer}',
    )(*operands)


def solution(mesh):
    row_axes = ('replica', 'dp')

    def local_step(x_rows, len_rows, cache, attn_gain, ffn_gain, w_query, w_attn_out, w_up, w_gate, w_down):
        layers, rows, _, kv_dim = cache.shape
        heads = w_query.shape[2] // kv_dim
        latent = w_attn_out.shape[1] // heads
        cache_t = jnp.swapaxes(cache, 2, 3)
        up_t, gate_t = jnp.swapaxes(w_up, 1, 2), jnp.swapaxes(w_gate, 1, 2)
        q = head(pltpu.with_memory_space_constraint(x_rows, pltpu.HBM), pltpu.with_memory_space_constraint(attn_gain, pltpu.HBM), w_query, heads)
        for layer in range(layers):
            mixed = attention(layer, q, len_rows, cache_t, rows, latent)
            next_q = (attn_gain, w_query, heads) if layer + 1 < layers else None
            outs = tail(layer, mixed, x_rows, ffn_gain, w_attn_out, gate_t, up_t, w_down, next_q)
            x_rows, q = outs[0], outs[-1]
        return x_rows

    return jax.shard_map(
        local_step,
        mesh=mesh,
        in_specs=(P(row_axes, None), P(row_axes), P(None, row_axes, None, None), P(), P(), P(), P(),
                  P(None, None, 'dp'), P(None, None, 'dp'), P(None, 'dp', None)),
        out_specs=P(row_axes, None),
        check_vma=False,
    )
```
